32 devices in a mesh: rep: 2 (over x), fsdp: 4 (over z), ep: 4 (over y, core).
Axes of the slice: x: 2, y: 2, z: 4, core: 2. Of those that a mesh axis runs over, the one named last changes fastest.
Arguments:
- tokens: bfloat16 [16384, 768], P(('rep', 'ep', 'fsdp')), parts along dimension 0
- expert_idx: int32 [16384, 1], P(('rep', 'ep', 'fsdp')), parts along dimension 0
- gates: float32 [16384, 1], P(('rep', 'ep', 'fsdp')), parts along dimension 0
- w_gate: bfloat16 [16, 768, 3072], P('ep', 'fsdp')
- w_up: bfloat16 [16, 768, 3072], P('ep', 'fsdp')
- w_down: bfloat16 [16, 3072, 768], P('ep', None, 'fsdp')
Outputs:
- output: bfloat16 [16384, 768], P(('rep', 'ep', 'fsdp')), parts along dimension 0
There are 2 independent parts. The reference program is written for one: setup_inputs(seed, part) draws one part's arguments, and reference() takes and returns one part's arrays. A program takes and returns all parts, laid end to end along the dimension named above; an argument that names none is the same for every part.
All inputs are finite; a program needn't handle non-finite values.
Results may differ from the reference program's by a relative error of at most 0.001.
Values are sent between devices in bfloat16 or wider.
A program may use at most 1 GiB of HBM per device.

```python
import jax
import jax.numpy as jnp
from jax import lax

TOK_DEV = 512
MODEL_DIM = 768
FFN_DIM = 3072
NUM_EXPERTS = 16
TOP_K = 1
EP_SIZE = 4
FSDP_SIZE = 4

GROUP_DEVS = EP_SIZE * FSDP_SIZE
ROW_COUNT = GROUP_DEVS * TOK_DEV
CAPACITY = (2 * TOK_DEV * TOP_K + NUM_EXPERTS - 1) // NUM_EXPERTS


def route_draw(key):
    key_rank, key_noise = jax.random.split(key)
    ranks = jax.random.permutation(key_rank, NUM_EXPERTS)
    skew = (ranks * 768) // NUM_EXPERTS
    noise = jax.random.randint(key_noise, (ROW_COUNT, NUM_EXPERTS), 0, 1024)
    scores = (noise + skew[None, :]) * NUM_EXPERTS + jnp.arange(NUM_EXPERTS)[None, :]
    top_vals, chosen = lax.top_k(scores, TOP_K)
    return chosen.astype(jnp.int32)


def setup_inputs(seed: int = 0, part: int = 0) -> dict:
    part_key = jax.random.fold_in(jax.random.key(seed), part)
    key_tok, key_route, key_gate = jax.random.split(part_key, 3)
    key_wg, key_wu, key_wd = jax.random.split(jax.random.key(seed + 1), 3)
    tokens = jax.random.normal(key_tok, (ROW_COUNT, MODEL_DIM), jnp.float32).astype(jnp.bfloat16)
    expert_idx = route_draw(key_route)
    gates = jax.random.uniform(key_gate, (ROW_COUNT, TOP_K), jnp.float32, 0.2, 0.8)
    w_gate = (jax.random.normal(key_wg, (NUM_EXPERTS, MODEL_DIM, FFN_DIM), jnp.float32) * MODEL_DIM ** -0.5).astype(jnp.bfloat16)
    w_up = (jax.random.normal(key_wu, (NUM_EXPERTS, MODEL_DIM, FFN_DIM), jnp.float32) * MODEL_DIM ** -0.5).astype(jnp.bfloat16)
    w_down = (jax.random.normal(key_wd, (NUM_EXPERTS, FFN_DIM, MODEL_DIM), jnp.float32) * (2.0 * FFN_DIM ** -0.5)).astype(jnp.bfloat16)
    return {'tokens': tokens, 'expert_idx': expert_idx, 'gates': gates, 'w_gate': w_gate, 'w_up': w_up, 'w_down': w_down}


def block_slots(idx_block):
    flat_ids = idx_block.reshape(TOK_DEV * TOP_K)
    onehot = (flat_ids[:, None] == jnp.arange(NUM_EXPERTS)[None, :]).astype(jnp.int32)
    before = jnp.cumsum(onehot, axis=0) - onehot
    return jnp.sum(before * onehot, axis=1)


def reference(tokens, expert_idx, gates, w_gate, w_up, w_down):
    pair_count = ROW_COUNT * TOP_K
    slot_ids = lax.map(block_slots, expert_idx.reshape(GROUP_DEVS, TOK_DEV, TOP_K)).reshape(pair_count)
    flat_ids = expert_idx.reshape(pair_count)
    pair_pos = jnp.arange(pair_count)
    block_id = pair_pos // (TOK_DEV * TOP_K)
    tok_row = (pair_pos // TOP_K).astype(jnp.int32)
    per_expert = GROUP_DEVS * CAPACITY
    total_rows = NUM_EXPERTS * per_expert
    target = jnp.where(slot_ids < CAPACITY, flat_ids * per_expert + block_id * CAPACITY + slot_ids, total_rows)
    row_of = jnp.full((total_rows,), ROW_COUNT, jnp.int32).at[target].set(tok_row, mode='drop')
    gate_of = jnp.zeros((total_rows,), jnp.float32).at[target].set(gates.reshape(pair_count), mode='drop')
    padded = jnp.concatenate([tokens, jnp.zeros((1, MODEL_DIM), tokens.dtype)], axis=0)

    def expert_step(acc, stacked):
        wg_one, wu_one, wd_one, rows_one, gate_one = stacked
        picked = padded[rows_one]
        act_a = jnp.dot(picked, wg_one, preferred_element_type=jnp.float32)
        act_b = jnp.dot(picked, wu_one, preferred_element_type=jnp.float32)
        hidden = (jax.nn.silu(act_a) * act_b).astype(jnp.bfloat16)
        expert_out = jnp.dot(hidden, wd_one, preferred_element_type=jnp.float32).astype(jnp.bfloat16)
        acc = acc.at[rows_one].add(gate_one[:, None] * expert_out.astype(jnp.float32), mode='drop')
        return acc, None

    acc_init = jnp.zeros((ROW_COUNT, MODEL_DIM), jnp.float32)
    acc, unused = lax.scan(expert_step, acc_init, (w_gate, w_up, w_down, row_of.reshape(NUM_EXPERTS, per_expert), gate_of.reshape(NUM_EXPERTS, per_expert)))
    return (tokens.astype(jnp.float32) + acc).astype(jnp.bfloat16)
```

```python
import functools

import jax
import jax.numpy as jnp
from jax import lax
from jax.experimental import pallas as pl
from jax.experimental.pallas import tpu as pltpu
from jax.sharding import PartitionSpec as P

MESH = pl.DeviceIdType.MESH
CHUNKS = 8
AHEAD = 4
ROW_BLOCKS = 4


def moe_kernel(n_ep, n_z, cap, chunks, ahead, row_blocks, idx_ref, gate_ref, tok_ref, wg_ref, wu_ref, wd_ref, out_ref,
               tok_v, send_v, x_v, o_v, back_v, acc_v, sel_v, w_v,
               tok_sem, own_sem, wsend_sem, wrecv_sem, xsend_sem, xrecv_sem, bsend_sem, brecv_sem):
    ep = lax.axis_index("ep")
    z = lax.axis_index("fsdp")
    me = ep * n_z + z
    n_dev = n_ep * n_z
    weights = (wg_ref, wu_ref, wd_ref)
    part, ffn = wg_ref.shape[1], wg_ref.shape[2]
    tok_count, dim = tok_ref.shape
    width = ffn // chunks
    slots = n_dev * cap
    block = slots // row_blocks
    per_block = n_dev // row_blocks

    def peer(d):
        other = lax.rem(me + d, n_dev)
        return other, {"ep": lax.div(other, n_z), "fsdp": lax.rem(other, n_z)}

    tok_copy = pltpu.make_async_copy(tok_ref, tok_v, tok_sem)
    tok_copy.start()
    own_copies = []
    for k in range(3):
        rows = pl.ds(pl.multiple_of(z * part, part), part)
        own_copies.append(pltpu.make_async_copy(weights[k].at[z], w_v.at[k, rows, :], own_sem.at[k]))
        own_copies[-1].start()

    barrier = pltpu.get_barrier_semaphore()
    for d in range(1, n_dev):
        pl.semaphore_signal(barrier, inc=1, device_id=peer(d)[1], device_id_type=MESH)
    pl.semaphore_wait(barrier, n_dev - 1)

    def weight_copy(k, d, c, cols):
        zp = lax.rem(z + d, n_z)
        rows = pl.ds(pl.multiple_of(z * part, part), part)
        return pltpu.make_async_remote_copy(
            src_ref=weights[k].at[zp, :, cols],
            dst_ref=w_v.at[k, rows, cols],
            send_sem=wsend_sem.at[k, d - 1],
            recv_sem=wrecv_sem.at[c, k, z],
            device_id={"fsdp": zp},
            device_id_type=MESH,
        )

    def send_weights(c):
        cols = pl.ds(c * width, width)
        for k in range(3):
            for d in range(1, n_z):
                weight_copy(k, d, c, cols).start()

    def wait_weights(c):
        cols = pl.ds(c * width, width)
        for k in range(3):
            for d in range(1, n_z):
                src = lax.rem(z + d, n_z)
                rows = pl.ds(pl.multiple_of(src * part, part), part)
                pltpu.make_async_remote_copy(
                    src_ref=weights[k].at[z, :, cols],
                    dst_ref=w_v.at[k, rows, cols],
                    send_sem=wsend_sem.at[k, d - 1],
                    recv_sem=wrecv_sem.at[c, k, src],
                    device_id={"fsdp": src},
                    device_id_type=MESH,
                ).wait_recv()

    send_weights(0)

    ids = idx_ref[...]
    onehot = (lax.broadcasted_iota(jnp.int32, (n_dev, tok_count), 0) == ids).astype(jnp.float32)
    earlier = (lax.broadcasted_iota(jnp.int32, (tok_count, tok_count), 0)
               < lax.broadcasted_iota(jnp.int32, (tok_count, tok_count), 1)).astype(jnp.bfloat16)
    before = jnp.dot(onehot.astype(jnp.bfloat16), earlier, preferred_element_type=jnp.float32)
    slot = jnp.sum(before * onehot, axis=0, keepdims=True)
    target = jnp.where(slot < cap, ids.astype(jnp.float32) * cap + slot, -1.0)

    tok_copy.wait()

    def dispatch(i, carry):
        first = i * block
        want = lax.broadcasted_iota(jnp.int32, (block, tok_count), 0) + first
        pick = (want.astype(jnp.float32) == target).astype(jnp.bfloat16)
        picked = jnp.dot(pick, tok_v[...], preferred_element_type=jnp.float32).astype(jnp.bfloat16)
        send_v[pl.ds(i * per_block, per_block)] = picked.reshape(per_block, cap, dim)
        return carry

    lax.fori_loop(0, row_blocks, dispatch, 0)

    lane = 128
    spread = jnp.transpose(jnp.broadcast_to(target, (lane, tok_count)))
    for j in range(slots // lane):
        want = lax.broadcasted_iota(jnp.int32, (tok_count, lane), 1) + j * lane
        sel_v[:, j * lane:(j + 1) * lane] = (spread == want.astype(jnp.float32)).astype(jnp.bfloat16)

    def row_copy(d):
        other, where = peer(d)
        return pltpu.make_async_remote_copy(
            src_ref=send_v.at[other],
            dst_ref=x_v.at[me],
            send_sem=xsend_sem.at[d],
            recv_sem=xrecv_sem.at[me],
            device_id=where,
            device_id_type=MESH,
        )

    def start_rows(d, carry):
        row_copy(d).start()
        return carry

    lax.fori_loop(1, n_dev, start_rows, 0)
    x_v[me] = send_v[me]

    for c in range(1, min(ahead, chunks)):
        send_weights(c)

    acc_v[...] = jnp.zeros_like(acc_v)
    for k in range(3):
        own_copies[k].wait()

    def wait_rows(d, carry):
        other, where = peer(d)
        pltpu.make_async_remote_copy(
            src_ref=send_v.at[other],
            dst_ref=x_v.at[other],
            send_sem=xsend_sem.at[d],
            recv_sem=xrecv_sem.at[other],
            device_id=where,
            device_id_type=MESH,
        ).wait()
        return carry

    def back_copy(s, where):
        return pltpu.make_async_remote_copy(
            src_ref=o_v.at[s],
            dst_ref=back_v.at[me],
            send_sem=bsend_sem.at[s],
            recv_sem=brecv_sem.at[me],
            device_id=where,
            device_id_type=MESH,
        )

    def chunk_rows(c, i):
        cols = slice(c * width, (c + 1) * width)
        x = x_v[pl.ds(i * per_block, per_block)].reshape(block, dim)
        a = jnp.dot(x, w_v[0, :, cols], preferred_element_type=jnp.float32)
        b = jnp.dot(x, w_v[1, :, cols], preferred_element_type=jnp.float32)
        h = (a * jax.nn.sigmoid(a) * b).astype(jnp.bfloat16)
        rows = pl.ds(pl.multiple_of(i * block, block), block)
        part_sum = lax.dot_general(h, w_v[2, :, cols], (((1,), (1,)), ((), ())), preferred_element_type=jnp.float32)
        return rows, acc_v[rows, :] + part_sum

    for c in range(chunks):
        wait_weights(c)
        if c + ahead < chunks:
            send_weights(c + ahead)
        if c == 0:
            lax.fori_loop(1, n_dev, wait_rows, 0)

        def body(i, carry, c=c):
            rows, total = chunk_rows(c, i)
            if c < chunks - 1:
                acc_v[rows, :] = total
            else:
                o_v[pl.ds(i * per_block, per_block)] = total.astype(jnp.bfloat16).reshape(per_block, cap, dim)
            return carry

        lax.fori_loop(0, row_blocks, body, 0)

    def start_back(d, carry):
        other, where = peer(d)
        back_copy(other, where).start()
        return carry

    lax.fori_loop(1, n_dev, start_back, 0)
    back_v[me] = o_v[me]

    for k in range(3):
        for d in range(1, n_z):
            zp = lax.rem(z + d, n_z)
            rows = pl.ds(pl.multiple_of(z * part, part), part)
            pltpu.make_async_remote_copy(
                src_ref=weights[k].at[zp],
                dst_ref=w_v.at[k, rows, :],
                send_sem=wsend_sem.at[k, d - 1],
                recv_sem=wrecv_sem.at[0, k, z],
                device_id={"fsdp": zp},
                device_id_type=MESH,
            ).wait_send()

    def wait_back(d, carry):
        other, where = peer(d)
        pltpu.make_async_remote_copy(
            src_ref=o_v.at[other],
            dst_ref=back_v.at[other],
            send_sem=bsend_sem.at[other],
            recv_sem=brecv_sem.at[other],
            device_id=where,
            device_id_type=MESH,
        ).wait()
        return carry

    lax.fori_loop(1, n_dev, wait_back, 0)

    mixed = jnp.dot(sel_v[...], back_v[...].reshape(slots, dim), preferred_element_type=jnp.float32)
    scale = jnp.transpose(jnp.broadcast_to(gate_ref[...], (lane, tok_count)))[:, :1]
    out_ref[...] = (tok_v[...].astype(jnp.float32) + scale * mixed).astype(jnp.bfloat16)


def solution(mesh):
    n_ep, n_z = mesh.shape["ep"], mesh.shape["fsdp"]
    row_spec = P(("rep", "ep", "fsdp"), None)

    def device_step(tokens, expert_idx, gates, w_gate, w_up, w_down):
        tok_count, top_k = expert_idx.shape
        assert top_k == 1 and w_gate.shape[0] == n_z
        dim = tokens.shape[1]
        n_local, part, ffn = w_gate.shape
        n_dev = n_ep * n_z
        cap = (2 * tok_count + n_dev - 1) // n_dev
        slots = n_dev * cap
        any_spec = pl.BlockSpec(memory_space=pl.ANY)
        vmem_spec = pl.BlockSpec(memory_space=pltpu.VMEM)
        dma = pltpu.SemaphoreType.DMA
        flops = 6 * slots * dim * ffn
        return pl.pallas_call(
            functools.partial(moe_kernel, n_ep, n_z, cap, CHUNKS, AHEAD, ROW_BLOCKS),
            out_shape=jax.ShapeDtypeStruct((tok_count, dim), jnp.bfloat16),
            in_specs=[vmem_spec, vmem_spec, any_spec, any_spec, any_spec, any_spec],
            out_specs=vmem_spec,
            scratch_shapes=[
                pltpu.VMEM((tok_count, dim), jnp.bfloat16),
                pltpu.VMEM((n_dev, cap, dim), jnp.bfloat16),
                pltpu.VMEM((n_dev, cap, dim), jnp.bfloat16),
                pltpu.VMEM((n_dev, cap, dim), jnp.bfloat16),
                pltpu.VMEM((n_dev, cap, dim), jnp.bfloat16),
                pltpu.VMEM((slots, dim), jnp.float32),
                pltpu.VMEM((tok_count, slots), jnp.bfloat16),
                pltpu.VMEM((3, n_z * part, ffn), jnp.bfloat16),
                dma, dma((3,)), dma((3, n_z - 1)), dma((CHUNKS, 3, n_z)),
                dma((n_dev,)), dma((n_dev,)), dma((n_dev,)), dma((n_dev,)),
            ],
            compiler_params=pltpu.CompilerParams(
                collective_id=0, has_side_effects=True, vmem_limit_bytes=60 * 1024 * 1024
            ),
            cost_estimate=pl.CostEstimate(flops=flops, bytes_accessed=6 * dim * ffn, transcendentals=slots * ffn),
        )(expert_idx.reshape(1, tok_count), gates.reshape(1, tok_count), tokens, w_gate, w_up, jnp.swapaxes(w_down, 1, 2))

    return jax.shard_map(
        device_step, mesh=mesh,
        in_specs=(row_spec, row_spec, row_spec, P("ep", "fsdp", None), P("ep", "fsdp", None), P("ep", None, "fsdp")),
        out_specs=row_spec, check_vma=False)
```

```python
import functools

import jax
import jax.numpy as jnp
from jax import lax
from jax.experimental import pallas as pl
from jax.experimental.pallas import tpu as pltpu
from jax.sharding import PartitionSpec as P

MESH = pl.DeviceIdType.MESH
WIDTHS = (3, 3, 3, 3, 3, 3, 3, 2, 1)
AHEAD = 4
ROW_BLOCKS = 4


def column_chunks(ffn):
    unit = ffn // sum(WIDTHS)
    starts = [sum(WIDTHS[:i]) * unit for i in range(len(WIDTHS))]
    return tuple((start, width * unit) for start, width in zip(starts, WIDTHS))


def moe_kernel(n_rep, n_ep, n_z, cap, chunks, ahead, row_blocks, idx_ref, gate_ref, tok_ref, wg_ref, wu_ref, wd_ref, out_ref,
               tok_v, send_v, x_v, o_v, back_v, acc_v, sel_v, w_v,
               tok_sem, own_sem, wsend_sem, wrecv_sem, fsend_sem, frecv_sem, xsend_sem, xrecv_sem, bsend_sem, brecv_sem):
    rep = lax.axis_index("rep")
    ep = lax.axis_index("ep")
    z = lax.axis_index("fsdp")
    me = ep * n_z + z
    n_dev = n_ep * n_z
    weights = (wg_ref, wu_ref, wd_ref)
    part = wg_ref.shape[1]
    share = part // n_rep
    tok_count, dim = tok_ref.shape
    slots = n_dev * cap
    block = slots // row_blocks
    per_block = n_dev // row_blocks

    def peer(d):
        other = lax.rem(me + d, n_dev)
        return other, {"ep": lax.div(other, n_z), "fsdp": lax.rem(other, n_z)}

    tok_copy = pltpu.make_async_copy(tok_ref, tok_v, tok_sem)
    tok_copy.start()
    own_copies = []
    for k in range(3):
        rows = pl.ds(pl.multiple_of(z * part, part), part)
        own_copies.append(pltpu.make_async_copy(weights[k].at[z], w_v.at[k, rows, :], own_sem.at[k]))
        own_copies[-1].start()

    barrier = pltpu.get_barrier_semaphore()
    for d in range(1, n_dev):
        pl.semaphore_signal(barrier, inc=1, device_id=peer(d)[1], device_id_type=MESH)
    for d in range(1, n_rep):
        pl.semaphore_signal(barrier, inc=1, device_id={"rep": lax.rem(rep + d, n_rep)}, device_id_type=MESH)
    pl.semaphore_wait(barrier, n_dev - 1 + n_rep - 1)

    def share_rows(src, of_rep):
        return pl.ds(pl.multiple_of(src * part + of_rep * share, share), share)

    def weight_copy(k, d, cols, sem):
        zp = lax.rem(z + d, n_z)
        return pltpu.make_async_remote_copy(
            src_ref=weights[k].at[zp, pl.ds(pl.multiple_of(rep * share, share), share), cols],
            dst_ref=w_v.at[k, share_rows(z, rep), cols],
            send_sem=wsend_sem.at[k, d - 1],
            recv_sem=sem,
            device_id={"fsdp": zp},
            device_id_type=MESH,
        )

    def send_weights(c):
        cols = pl.ds(*chunks[c])
        for k in range(3):
            for d in range(1, n_z):
                weight_copy(k, d, cols, wrecv_sem.at[c, k, z]).start()

    def pass_copy(k, src, of_rep, cols, sem):
        return pltpu.make_async_remote_copy(
            src_ref=w_v.at[k, share_rows(src, of_rep), cols],
            dst_ref=w_v.at[k, share_rows(src, of_rep), cols],
            send_sem=fsend_sem.at[k, src],
            recv_sem=sem,
            device_id={"rep": lax.rem(rep + 1, n_rep)},
            device_id_type=MESH,
        )

    def receive_weights(c):
        cols = pl.ds(*chunks[c])
        for k in range(3):
            for d in range(1, n_z):
                src = lax.rem(z + d, n_z)
                pltpu.make_async_remote_copy(
                    src_ref=w_v.at[k, share_rows(src, rep), cols],
                    dst_ref=w_v.at[k, share_rows(src, rep), cols],
                    send_sem=wsend_sem.at[k, d - 1],
                    recv_sem=wrecv_sem.at[c, k, src],
                    device_id={"fsdp": src},
                    device_id_type=MESH,
                ).wait_recv()
                if n_rep > 1:
                    pass_copy(k, src, rep, cols, frecv_sem.at[c, k, src]).start()

    def wait_passed(c):
        cols = pl.ds(*chunks[c])
        if n_rep > 1:
            for k in range(3):
                for d in range(1, n_z):
                    src = lax.rem(z + d, n_z)
                    pass_copy(k, src, lax.rem(rep + 1, n_rep), cols, frecv_sem.at[c, k, src]).wait_recv()

    send_weights(0)

    ids = idx_ref[...]
    onehot = (lax.broadcasted_iota(jnp.int32, (n_dev, tok_count), 0) == ids).astype(jnp.float32)
    earlier = (lax.broadcasted_iota(jnp.int32, (tok_count, tok_count), 0)
               < lax.broadcasted_iota(jnp.int32, (tok_count, tok_count), 1)).astype(jnp.bfloat16)
    before = jnp.dot(onehot.astype(jnp.bfloat16), earlier, preferred_element_type=jnp.float32)
    slot = jnp.sum(before * onehot, axis=0, keepdims=True)
    target = jnp.where(slot < cap, ids.astype(jnp.float32) * cap + slot, -1.0)

    tok_copy.wait()

    def dispatch(i, carry):
        first = i * block
        want = lax.broadcasted_iota(jnp.int32, (block, tok_count), 0) + first
        pick = (want.astype(jnp.float32) == target).astype(jnp.bfloat16)
        picked = jnp.dot(pick, tok_v[...], preferred_element_type=jnp.float32).astype(jnp.bfloat16)
        send_v[pl.ds(i * per_block, per_block)] = picked.reshape(per_block, cap, dim)
        return carry

    lax.fori_loop(0, row_blocks, dispatch, 0)

    lane = 128
    spread = jnp.transpose(jnp.broadcast_to(target, (lane, tok_count)))
    for j in range(slots // lane):
        want = lax.broadcasted_iota(jnp.int32, (tok_count, lane), 1) + j * lane
        sel_v[:, j * lane:(j + 1) * lane] = (spread == want.astype(jnp.float32)).astype(jnp.bfloat16)

    def row_copy(d):
        other, where = peer(d)
        return pltpu.make_async_remote_copy(
            src_ref=send_v.at[other],
            dst_ref=x_v.at[me],
            send_sem=xsend_sem.at[d],
            recv_sem=xrecv_sem.at[me],
            device_id=where,
            device_id_type=MESH,
        )

    def start_rows(d, carry):
        row_copy(d).start()
        return carry

    lax.fori_loop(1, n_dev, start_rows, 0)
    x_v[me] = send_v[me]

    for c in range(1, min(ahead, len(chunks))):
        send_weights(c)

    acc_v[...] = jnp.zeros_like(acc_v)
    for k in range(3):
        own_copies[k].wait()

    def wait_rows(d, carry):
        other, where = peer(d)
        pltpu.make_async_remote_copy(
            src_ref=send_v.at[other],
            dst_ref=x_v.at[other],
            send_sem=xsend_sem.at[d],
            recv_sem=xrecv_sem.at[other],
            device_id=where,
            device_id_type=MESH,
        ).wait()
        return carry

    def back_copy(s, where):
        return pltpu.make_async_remote_copy(
            src_ref=o_v.at[s],
            dst_ref=back_v.at[me],
            send_sem=bsend_sem.at[s],
            recv_sem=brecv_sem.at[me],
            device_id=where,
            device_id_type=MESH,
        )

    def compute(c):
        start, width = chunks[c]
        cols = slice(start, start + width)
        last = c == len(chunks) - 1

        def start_back(i):
            for j in range(per_block):
                s = i * per_block + j

                @pl.when(s != me)
                def _():
                    back_copy(s, {"ep": lax.div(s, n_z), "fsdp": lax.rem(s, n_z)}).start()

        def body(n, carry):
            i = lax.rem(ep + n, row_blocks)
            x = x_v[pl.ds(i * per_block, per_block)].reshape(block, dim)
            a = jnp.dot(x, w_v[0, :, cols], preferred_element_type=jnp.float32)
            b = jnp.dot(x, w_v[1, :, cols], preferred_element_type=jnp.float32)
            h = (a * jax.nn.sigmoid(a) * b).astype(jnp.bfloat16)
            rows = pl.ds(pl.multiple_of(i * block, block), block)
            total = acc_v[rows, :] + lax.dot_general(
                h, w_v[2, :, cols], (((1,), (1,)), ((), ())), preferred_element_type=jnp.float32)
            if last:
                o_v[pl.ds(i * per_block, per_block)] = total.astype(jnp.bfloat16).reshape(per_block, cap, dim)

                @pl.when(n > 0)
                def _():
                    start_back(lax.rem(ep + n + row_blocks - 1, row_blocks))
            else:
                acc_v[rows, :] = total
            return carry

        lax.fori_loop(0, row_blocks, body, 0)
        if last:
            back_v[me] = o_v[me]
            start_back(lax.rem(ep + row_blocks - 1, row_blocks))

    for c in range(len(chunks)):
        receive_weights(c)
        if c + ahead < len(chunks):
            send_weights(c + ahead)
        if c == 0:
            lax.fori_loop(1, n_dev, wait_rows, 0)
        else:
            wait_passed(c - 1)
            compute(c - 1)
    wait_passed(len(chunks) - 1)
    compute(len(chunks) - 1)

    whole = pl.ds(0, sum(width for _, width in chunks))
    for k in range(3):
        for d in range(1, n_z):
            weight_copy(k, d, whole, wrecv_sem.at[0, k, z]).wait_send()
            if n_rep > 1:
                src = lax.rem(z + d, n_z)
                pass_copy(k, src, rep, whole, frecv_sem.at[0, k, src]).wait_send()

    def wait_back(d, carry):
        other, where = peer(d)
        pltpu.make_async_remote_copy(
            src_ref=o_v.at[other],
            dst_ref=back_v.at[other],
            send_sem=bsend_sem.at[other],
            recv_sem=brecv_sem.at[other],
            device_id=where,
            device_id_type=MESH,
        ).wait()
        return carry

    lax.fori_loop(1, n_dev, wait_back, 0)

    mixed = jnp.dot(sel_v[...], back_v[...].reshape(slots, dim), preferred_element_type=jnp.float32)
    scale = jnp.transpose(jnp.broadcast_to(gate_ref[...], (lane, tok_count)))[:, :1]
    out_ref[...] = (tok_v[...].astype(jnp.float32) + scale * mixed).astype(jnp.bfloat16)


def solution(mesh):
    n_rep, n_ep, n_z = mesh.shape["rep"], mesh.shape["ep"], mesh.shape["fsdp"]
    row_spec = P(("rep", "ep", "fsdp"), None)

    def device_step(tokens, expert_idx, gates, w_gate, w_up, w_down):
        tok_count, top_k = expert_idx.shape
        assert top_k == 1 and w_gate.shape[0] == n_z and n_rep <= 2 and n_ep == ROW_BLOCKS
        dim = tokens.shape[1]
        n_local, part, ffn = w_gate.shape
        n_dev = n_ep * n_z
        cap = (2 * tok_count + n_dev - 1) // n_dev
        slots = n_dev * cap
        any_spec = pl.BlockSpec(memory_space=pl.ANY)
        vmem_spec = pl.BlockSpec(memory_space=pltpu.VMEM)
        dma = pltpu.SemaphoreType.DMA
        chunks = column_chunks(ffn)
        flops = 6 * slots * dim * ffn
        return pl.pallas_call(
            functools.partial(moe_kernel, n_rep, n_ep, n_z, cap, chunks, AHEAD, ROW_BLOCKS),
            out_shape=jax.ShapeDtypeStruct((tok_count, dim), jnp.bfloat16),
            in_specs=[vmem_spec, vmem_spec, any_spec, any_spec, any_spec, any_spec],
            out_specs=vmem_spec,
            scratch_shapes=[
                pltpu.VMEM((tok_count, dim), jnp.bfloat16),
                pltpu.VMEM((n_dev, cap, dim), jnp.bfloat16),
                pltpu.VMEM((n_dev, cap, dim), jnp.bfloat16),
                pltpu.VMEM((n_dev, cap, dim), jnp.bfloat16),
                pltpu.VMEM((n_dev, cap, dim), jnp.bfloat16),
                pltpu.VMEM((slots, dim), jnp.float32),
                pltpu.VMEM((tok_count, slots), jnp.bfloat16),
                pltpu.VMEM((3, n_z * part, ffn), jnp.bfloat16),
                dma, dma((3,)), dma((3, n_z - 1)), dma((len(chunks), 3, n_z)), dma((3, n_z)), dma((len(chunks), 3, n_z)),
                dma((n_dev,)), dma((n_dev,)), dma((n_dev,)), dma((n_dev,)),
            ],
            compiler_params=pltpu.CompilerParams(
                collective_id=0, has_side_effects=True, vmem_limit_bytes=60 * 1024 * 1024
            ),
            cost_estimate=pl.CostEstimate(flops=flops, bytes_accessed=6 * dim * ffn, transcendentals=slots * ffn),
        )(expert_idx.reshape(1, tok_count), gates.reshape(1, tok_count), tokens, w_gate, w_up, jnp.swapaxes(w_down, 1, 2))

    return jax.shard_map(
        device_step, mesh=mesh,
        in_specs=(row_spec, row_spec, row_spec, P("ep", "fsdp", None), P("ep", "fsdp", None), P("ep", None, "fsdp")),
        out_specs=row_spec, check_vma=False)
```

```python
import functools

import jax
import jax.numpy as jnp
from jax import lax
from jax.experimental import pallas as pl
from jax.experimental.pallas import tpu as pltpu
from jax.sharding import PartitionSpec as P

MESH = pl.DeviceIdType.MESH
LANE = 128
HALF = 64
CHUNKS = 6
AHEAD = 3
ROW_BLOCKS = 4


def aligned(start, size, step):
    return pl.ds(pl.multiple_of(start * step, step), size)


def moe_kernel(n_rep, n_ep, n_z, cap, idx_ref, gate_ref, tok_ref, wg_ref, wu_ref, wd_ref, out_ref,
               tok_v, send_v, x_v, w_v, wd0_v, wd1_v, h_v, o0_v, o1_v, back0_v, back1_v, sel_v,
               tok_sem, own_sem, gsend, grecv, gpass_send, gpass_recv, dsend, drecv, dpass_send, dpass_recv,
               xsend, xrecv, bsend, brecv):
    rep, ep, z = lax.axis_index("rep"), lax.axis_index("ep"), lax.axis_index("fsdp")
    rep = rep if n_rep > 1 else 0
    me = ep * n_z + z
    n_dev = n_ep * n_z
    part, ffn = wg_ref.shape[1], wg_ref.shape[2]
    share, span = part // n_rep, ffn // n_rep
    width = ffn // CHUNKS
    tok_count, dim = tok_ref.shape
    slots = n_dev * cap
    block, per_block = slots // ROW_BLOCKS, n_dev // ROW_BLOCKS
    gate_up = (wg_ref, wu_ref)
    wd_v, o_v, back_v = (wd0_v, wd1_v), (o0_v, o1_v), (back0_v, back1_v)
    group_rows = ((0, LANE), (LANE, HALF))
    other_rep = {"rep": lax.rem(rep + 1, n_rep)}

    def place(s):
        return {"ep": lax.div(s, n_z), "fsdp": lax.rem(s, n_z)}

    def remote(src, dst, send_sem, recv_sem, where):
        return pltpu.make_async_remote_copy(
            src_ref=src, dst_ref=dst, send_sem=send_sem, recv_sem=recv_sem, device_id=where, device_id_type=MESH)

    local = [pltpu.make_async_copy(tok_ref, tok_v, tok_sem)]
    for k in range(2):
        local.append(pltpu.make_async_copy(gate_up[k].at[z], w_v.at[k, aligned(z, part, part), :], own_sem.at[k]))
    for g, (first, rows) in enumerate(group_rows):
        local.append(pltpu.make_async_copy(
            wd_ref.at[z, first:first + rows, :], wd_v[g].at[aligned(z, rows, rows), :], own_sem.at[2 + g]))
    for copy in local:
        copy.start()

    barrier = pltpu.get_barrier_semaphore()
    for d in range(1, n_dev):
        pl.semaphore_signal(barrier, inc=1, device_id=place(lax.rem(me + d, n_dev)), device_id_type=MESH)
    if n_rep > 1:
        pl.semaphore_signal(barrier, inc=1, device_id=other_rep, device_id_type=MESH)
    pl.semaphore_wait(barrier, n_dev - 1 + n_rep - 1)

    peers = [lax.rem(z + d, n_z) for d in range(1, n_z)]

    def share_rows(src, of_rep):
        return pl.ds(pl.multiple_of(src * part + of_rep * share, share), share)

    def gate_up_copy(k, p, cols, sem):
        zp = peers[p]
        return remote(gate_up[k].at[zp, aligned(rep, share, share), cols], w_v.at[k, share_rows(z, rep), cols],
                      gsend.at[k, p], sem, {"fsdp": zp})

    def gate_up_pass(src, of_rep, cols, sem):
        at = w_v.at[:, share_rows(src, of_rep), cols]
        return remote(at, at, gpass_send.at[src], sem, other_rep)

    def down_copy(g, p):
        zp = peers[p]
        first, rows = group_rows[g]
        cols = aligned(rep, span, span)
        return remote(wd_ref.at[zp, first:first + rows, cols], wd_v[g].at[aligned(z, rows, rows), cols],
                      dsend.at[g, p], drecv.at[g, z], {"fsdp": zp})

    def down_pass(g, src, of_rep):
        rows = group_rows[g][1]
        at = wd_v[g].at[aligned(src, rows, rows), aligned(of_rep, span, span)]
        return remote(at, at, dpass_send.at[g, src], dpass_recv.at[g, src], other_rep)

    def row_copy(s, at):
        return remote(send_v.at[s], x_v.at[at], xsend.at[s], xrecv.at[at], place(s))

    def back_copy(g, s, at):
        return remote(o_v[g].at[s], back_v[g].at[at], bsend.at[g, s], brecv.at[g, at], place(s))

    def for_others(run):
        def step(d, carry):
            run(lax.rem(me + d, n_dev))
            return carry
        lax.fori_loop(1, n_dev, step, 0)

    def send(item):
        if item < CHUNKS:
            cols = pl.ds(item * width, width)
            for p in range(n_z - 1):
                for k in range(2):
                    gate_up_copy(k, p, cols, grecv.at[item, k, z]).start()
        elif item == CHUNKS:
            for_others(lambda s: row_copy(s, me).start())
        elif item <= CHUNKS + 2:
            for p in range(n_z - 1):
                down_copy(item - CHUNKS - 1, p).start()

    def receive(item):
        if item < CHUNKS:
            cols = pl.ds(item * width, width)
            for src in peers:
                for k in range(2):
                    at = w_v.at[k, share_rows(src, rep), cols]
                    remote(at, at, gsend.at[k, 0], grecv.at[item, k, src], {"fsdp": src}).wait_recv()
                if n_rep > 1:
                    gate_up_pass(src, rep, cols, gpass_recv.at[item, src]).start()
        elif item == CHUNKS:
            for_others(lambda s: row_copy(s, s).wait())
        else:
            g = item - CHUNKS - 1
            for src in peers:
                rows = group_rows[g][1]
                at = wd_v[g].at[aligned(src, rows, rows), aligned(rep, span, span)]
                remote(at, at, dsend.at[g, 0], drecv.at[g, src], {"fsdp": src}).wait_recv()
                if n_rep > 1:
                    down_pass(g, src, rep).start()

    for item in range(AHEAD):
        send(item)

    ids = idx_ref[...]
    onehot = (lax.broadcasted_iota(jnp.int32, (n_dev, tok_count), 0) == ids).astype(jnp.float32)
    earlier = (lax.broadcasted_iota(jnp.int32, (tok_count, tok_count), 0)
               < lax.broadcasted_iota(jnp.int32, (tok_count, tok_count), 1)).astype(jnp.bfloat16)
    before = jnp.dot(onehot.astype(jnp.bfloat16), earlier, preferred_element_type=jnp.float32)
    slot = jnp.sum(before * onehot, axis=0, keepdims=True)
    target = jnp.where(slot < cap, ids.astype(jnp.float32) * cap + slot, -1.0)

    local[0].wait()

    def dispatch(i, carry):
        want = lax.broadcasted_iota(jnp.int32, (block, tok_count), 0) + i * block
        pick = (want.astype(jnp.float32) == target).astype(jnp.bfloat16)
        picked = jnp.dot(pick, tok_v[...], preferred_element_type=jnp.float32).astype(jnp.bfloat16)
        send_v[pl.ds(i * per_block, per_block)] = picked.reshape(per_block, cap, dim)
        return carry

    lax.fori_loop(0, ROW_BLOCKS, dispatch, 0)
    x_v[me] = send_v[me]

    spread = jnp.transpose(jnp.broadcast_to(target, (LANE, tok_count)))
    for j in range(slots // LANE):
        want = lax.broadcasted_iota(jnp.int32, (tok_count, LANE), 1) + j * LANE
        sel_v[:, j * LANE:(j + 1) * LANE] = (spread == want.astype(jnp.float32)).astype(jnp.bfloat16)

    for item in range(CHUNKS + 1):
        receive(item)
        send(item + AHEAD)

    for copy in local[1:]:
        copy.wait()
    for c in range(CHUNKS):
        cols = slice(c * width, (c + 1) * width)
        if n_rep > 1:
            for src in peers:
                gate_up_pass(src, 1 - rep, pl.ds(c * width, width), gpass_recv.at[c, src]).wait_recv()

        def hidden(i, carry, cols=cols):
            x = x_v[pl.ds(i * per_block, per_block)].reshape(block, dim)
            a = jnp.dot(x, w_v[0, :, cols], preferred_element_type=jnp.float32)
            b = jnp.dot(x, w_v[1, :, cols], preferred_element_type=jnp.float32)
            h_v[aligned(i, block, block), cols] = (a * jax.nn.sigmoid(a) * b).astype(jnp.bfloat16)
            return carry

        lax.fori_loop(0, ROW_BLOCKS, hidden, 0)

    def finish(g):
        if n_rep > 1:
            for src in peers:
                down_pass(g, src, 1 - rep).wait_recv()

        def send_back(i):
            for j in range(per_block):
                s = i * per_block + j

                @pl.when(s != me)
                def _():
                    back_copy(g, s, me).start()

        def rows_out(n, carry):
            i = lax.rem(ep + n, ROW_BLOCKS)
            total = lax.dot_general(h_v[aligned(i, block, block), :], wd_v[g][...], (((1,), (1,)), ((), ())),
                                    preferred_element_type=jnp.float32)
            o_v[g][pl.ds(i * per_block, per_block)] = total.astype(jnp.bfloat16).reshape(
                per_block, cap, n_z * group_rows[g][1])

            @pl.when(n > 0)
            def _():
                send_back(lax.rem(i + ROW_BLOCKS - 1, ROW_BLOCKS))

            return carry

        lax.fori_loop(0, ROW_BLOCKS, rows_out, 0)
        back_v[g][me] = o_v[g][me]
        send_back(lax.rem(ep + ROW_BLOCKS - 1, ROW_BLOCKS))

    receive(CHUNKS + 1)
    finish(0)
    receive(CHUNKS + 2)
    finish(1)

    every = pl.ds(0, ffn)
    for p in range(n_z - 1):
        for k in range(2):
            gate_up_copy(k, p, every, grecv.at[0, k, z]).wait_send()
        for g in range(2):
            down_copy(g, p).wait_send()
        if n_rep > 1:
            gate_up_pass(peers[p], rep, every, gpass_recv.at[0, peers[p]]).wait_send()
            for g in range(2):
                down_pass(g, peers[p], rep).wait_send()

    scale = jnp.transpose(jnp.broadcast_to(gate_ref[...], (LANE, tok_count)))
    low_lanes = lax.broadcasted_iota(jnp.int32, (tok_count, LANE), 1) < HALF
    mixed = []

    def piece(half):
        src, j = divmod(half, part // HALF)
        g, start = (0, src * LANE) if j < 2 else (1, (src // 2) * LANE)
        return mixed[g][:, start:start + LANE], j if j < 2 else src % 2

    def put(t):
        (low, low_at), (high, high_at) = piece(2 * t), piece(2 * t + 1)
        low = low if low_at == 0 else pltpu.roll(low, HALF, 1)
        high = high if high_at == 1 else pltpu.roll(high, HALF, 1)
        cols = slice(t * LANE, (t + 1) * LANE)
        value = jnp.where(low_lanes, low, high)
        out_ref[:, cols] = (tok_v[:, cols].astype(jnp.float32) + scale * value).astype(jnp.bfloat16)

    only_first = [t for t in range(dim // LANE) if (2 * t) % 3 < 2 and (2 * t + 1) % 3 < 2]
    for g in range(2):
        for_others(lambda s, g=g: back_copy(g, s, s).wait())
        mixed.append(jnp.dot(sel_v[...], back_v[g][...].reshape(slots, n_z * group_rows[g][1]),
                             preferred_element_type=jnp.float32))
        for t in range(dim // LANE):
            if (t in only_first) == (g == 0):
                put(t)


def solution(mesh):
    n_rep, n_ep, n_z = mesh.shape["rep"], mesh.shape["ep"], mesh.shape["fsdp"]
    row_spec = P(("rep", "ep", "fsdp"), None)

    def device_step(tokens, expert_idx, gates, w_gate, w_up, w_down):
        tok_count, top_k = expert_idx.shape
        n_local, part, ffn = w_gate.shape
        dim = tokens.shape[1]
        assert top_k == 1 and n_local == n_z and n_ep == ROW_BLOCKS and part == LANE + HALF and n_rep <= 2
        n_dev = n_ep * n_z
        cap = (2 * tok_count + n_dev - 1) // n_dev
        slots = n_dev * cap
        any_spec = pl.BlockSpec(memory_space=pl.ANY)
        vmem_spec = pl.BlockSpec(memory_space=pltpu.VMEM)
        dma, bf16 = pltpu.SemaphoreType.DMA, jnp.bfloat16
        return pl.pallas_call(
            functools.partial(moe_kernel, n_rep, n_ep, n_z, cap),
            out_shape=jax.ShapeDtypeStruct((tok_count, dim), bf16),
            in_specs=[vmem_spec, vmem_spec, any_spec, any_spec, any_spec, any_spec],
            out_specs=vmem_spec,
            scratch_shapes=[
                pltpu.VMEM((tok_count, dim), bf16),
                pltpu.VMEM((n_dev, cap, dim), bf16),
                pltpu.VMEM((n_dev, cap, dim), bf16),
                pltpu.VMEM((2, n_z * part, ffn), bf16),
                pltpu.VMEM((n_z * LANE, ffn), bf16),
                pltpu.VMEM((n_z * HALF, ffn), bf16),
                pltpu.VMEM((slots, ffn), bf16),
                pltpu.VMEM((n_dev, cap, n_z * LANE), bf16),
                pltpu.VMEM((n_dev, cap, n_z * HALF), bf16),
                pltpu.VMEM((n_dev, cap, n_z * LANE), bf16),
                pltpu.VMEM((n_dev, cap, n_z * HALF), bf16),
                pltpu.VMEM((tok_count, slots), bf16),
                dma, dma((4,)),
                dma((2, n_z - 1)), dma((CHUNKS, 2, n_z)), dma((n_z,)), dma((CHUNKS, n_z)),
                dma((2, n_z - 1)), dma((2, n_z)), dma((2, n_z)), dma((2, n_z)),
                dma((n_dev,)), dma((n_dev,)), dma((2, n_dev)), dma((2, n_dev)),
            ],
            compiler_params=pltpu.CompilerParams(
                collective_id=0, has_side_effects=True, vmem_limit_bytes=60 * 1024 * 1024),
            cost_estimate=pl.CostEstimate(
                flops=6 * slots * dim * ffn, bytes_accessed=6 * dim * ffn, transcendentals=slots * ffn),
        )(expert_idx.reshape(1, tok_count), gates.reshape(1, tok_count), tokens, w_gate, w_up, jnp.swapaxes(w_down, 1, 2))

    return jax.shard_map(
        device_step, mesh=mesh,
        in_specs=(row_spec, row_spec, row_spec, P("ep", "fsdp", None), P("ep", "fsdp", None), P("ep", None, "fsdp")),
        out_specs=row_spec, check_vma=False)
```

```python
import functools

import jax
import jax.numpy as jnp
from jax import lax
from jax.experimental import pallas as pl
from jax.experimental.pallas import tpu as pltpu
from jax.sharding import PartitionSpec as P

MESH = pl.DeviceIdType.MESH
LANE = 128
HALF = 64
CHUNKS = 6
AHEAD = 3
DOWN_SPLIT = 3
ROW_BLOCKS = 4


def aligned(start, size, step):
    return pl.ds(pl.multiple_of(start * step, step), size)


def moe_kernel(n_rep, n_ep, n_z, cap, idx_ref, gate_ref, tok_ref, wg_ref, wu_ref, wd_ref, out_ref,
               tok_v, send_v, x_v, w_v, wd0_v, wd1_v, h_v, o0_v, o1_v, back0_v, back1_v, sel_v,
               tok_sem, own_sem, gsend, grecv, gpass_send, gpass_recv, dsend, drecv, dpass_send, dpass_recv,
               xsend, xrecv, bsend, brecv):
    rep, ep, z = lax.axis_index("rep"), lax.axis_index("ep"), lax.axis_index("fsdp")
    rep = rep if n_rep > 1 else 0
    me = ep * n_z + z
    n_dev = n_ep * n_z
    part, ffn = wg_ref.shape[1], wg_ref.shape[2]
    share, span = part // n_rep, ffn // n_rep // DOWN_SPLIT
    width = ffn // CHUNKS
    tok_count, dim = tok_ref.shape
    slots = n_dev * cap
    block, per_block = slots // ROW_BLOCKS, n_dev // ROW_BLOCKS
    gate_up = (wg_ref, wu_ref)
    wd_v, o_v, back_v = (wd0_v, wd1_v), (o0_v, o1_v), (back0_v, back1_v)
    group_rows = ((0, LANE), (LANE, HALF))
    other_rep = {"rep": lax.rem(rep + 1, n_rep)}

    def place(s):
        return {"ep": lax.div(s, n_z), "fsdp": lax.rem(s, n_z)}

    def remote(src, dst, send_sem, recv_sem, where):
        return pltpu.make_async_remote_copy(
            src_ref=src, dst_ref=dst, send_sem=send_sem, recv_sem=recv_sem, device_id=where, device_id_type=MESH)

    local = [pltpu.make_async_copy(tok_ref, tok_v, tok_sem)]
    for k in range(2):
        local.append(pltpu.make_async_copy(gate_up[k].at[z], w_v.at[k, aligned(z, part, part), :], own_sem.at[k]))
    for g, (first, rows) in enumerate(group_rows):
        local.append(pltpu.make_async_copy(
            wd_ref.at[z, first:first + rows, :], wd_v[g].at[aligned(z, rows, rows), :], own_sem.at[2 + g]))
    for copy in local:
        copy.start()

    barrier = pltpu.get_barrier_semaphore()
    for d in range(1, n_dev):
        pl.semaphore_signal(barrier, inc=1, device_id=place(lax.rem(me + d, n_dev)), device_id_type=MESH)
    if n_rep > 1:
        pl.semaphore_signal(barrier, inc=1, device_id=other_rep, device_id_type=MESH)
    pl.semaphore_wait(barrier, n_dev - 1 + n_rep - 1)

    peers = [lax.rem(z + d, n_z) for d in range(1, n_z)]

    def share_rows(src, of_rep):
        return pl.ds(pl.multiple_of(src * part + of_rep * share, share), share)

    def gate_up_copy(k, p, cols, sem):
        zp = peers[p]
        return remote(gate_up[k].at[zp, aligned(rep, share, share), cols], w_v.at[k, share_rows(z, rep), cols],
                      gsend.at[k, p], sem, {"fsdp": zp})

    def gate_up_pass(src, of_rep, cols, sem):
        at = w_v.at[:, share_rows(src, of_rep), cols]
        return remote(at, at, gpass_send.at[src], sem, other_rep)

    def down_cols(of_rep, q):
        return aligned(of_rep * DOWN_SPLIT + q, span, span)

    def down_copy(g, q, p):
        zp = peers[p]
        first, rows = group_rows[g]
        cols = down_cols(rep, q)
        return remote(wd_ref.at[zp, first:first + rows, cols], wd_v[g].at[aligned(z, rows, rows), cols],
                      dsend.at[g, q, p], drecv.at[g, q, z], {"fsdp": zp})

    def down_pass(g, q, src, of_rep):
        rows = group_rows[g][1]
        at = wd_v[g].at[aligned(src, rows, rows), down_cols(of_rep, q)]
        return remote(at, at, dpass_send.at[g, q, src], dpass_recv.at[g, q, src], other_rep)

    def row_copy(s, at):
        return remote(send_v.at[s], x_v.at[at], xsend.at[s], xrecv.at[at], place(s))

    def back_copy(g, s, at):
        return remote(o_v[g].at[s], back_v[g].at[at], bsend.at[g, s], brecv.at[g, at], place(s))

    def for_others(run):
        def step(d, carry):
            run(lax.rem(me + d, n_dev))
            return carry
        lax.fori_loop(1, n_dev, step, 0)

    def send(item):
        if item < CHUNKS:
            cols = pl.ds(item * width, width)
            for p in range(n_z - 1):
                for k in range(2):
                    gate_up_copy(k, p, cols, grecv.at[item, k, z]).start()
        elif item == CHUNKS:
            for_others(lambda s: row_copy(s, me).start())
        elif item <= CHUNKS + 2 * DOWN_SPLIT:
            g, q = divmod(item - CHUNKS - 1, DOWN_SPLIT)
            for p in range(n_z - 1):
                down_copy(g, q, p).start()

    def receive(item):
        if item < CHUNKS:
            cols = pl.ds(item * width, width)
            for src in reversed(peers):
                for k in range(2):
                    at = w_v.at[k, share_rows(src, rep), cols]
                    remote(at, at, gsend.at[k, 0], grecv.at[item, k, src], {"fsdp": src}).wait_recv()
                if n_rep > 1:
                    gate_up_pass(src, rep, cols, gpass_recv.at[item, src]).start()
        elif item == CHUNKS:
            for_others(lambda s: row_copy(s, s).wait())
        else:
            g, q = divmod(item - CHUNKS - 1, DOWN_SPLIT)
            for src in reversed(peers):
                rows = group_rows[g][1]
                at = wd_v[g].at[aligned(src, rows, rows), down_cols(rep, q)]
                remote(at, at, dsend.at[g, q, 0], drecv.at[g, q, src], {"fsdp": src}).wait_recv()
                if n_rep > 1:
                    down_pass(g, q, src, rep).start()

    for item in range(AHEAD):
        send(item)

    ids = idx_ref[...]
    onehot = (lax.broadcasted_iota(jnp.int32, (n_dev, tok_count), 0) == ids).astype(jnp.float32)
    earlier = (lax.broadcasted_iota(jnp.int32, (tok_count, tok_count), 0)
               < lax.broadcasted_iota(jnp.int32, (tok_count, tok_count), 1)).astype(jnp.bfloat16)
    before = jnp.dot(onehot.astype(jnp.bfloat16), earlier, preferred_element_type=jnp.float32)
    slot = jnp.sum(before * onehot, axis=0, keepdims=True)
    target = jnp.where(slot < cap, ids.astype(jnp.float32) * cap + slot, -1.0)

    local[0].wait()

    def dispatch(i, carry):
        want = lax.broadcasted_iota(jnp.int32, (block, tok_count), 0) + i * block
        pick = (want.astype(jnp.float32) == target).astype(jnp.bfloat16)
        picked = jnp.dot(pick, tok_v[...], preferred_element_type=jnp.float32).astype(jnp.bfloat16)
        send_v[pl.ds(i * per_block, per_block)] = picked.reshape(per_block, cap, dim)
        return carry

    lax.fori_loop(0, ROW_BLOCKS, dispatch, 0)
    x_v[me] = send_v[me]

    spread = jnp.transpose(jnp.broadcast_to(target, (LANE, tok_count)))
    for j in range(slots // LANE):
        want = lax.broadcasted_iota(jnp.int32, (tok_count, LANE), 1) + j * LANE
        sel_v[:, j * LANE:(j + 1) * LANE] = (spread == want.astype(jnp.float32)).astype(jnp.bfloat16)

    items = iter(range(CHUNKS + 1 + 2 * DOWN_SPLIT))

    def receive_next():
        item = next(items)
        receive(item)
        send(item + AHEAD)

    for _ in range(CHUNKS + 1):
        receive_next()

    for copy in local[1:]:
        copy.wait()
    for c in range(CHUNKS):
        cols = slice(c * width, (c + 1) * width)
        if n_rep > 1:
            for src in peers:
                gate_up_pass(src, 1 - rep, pl.ds(c * width, width), gpass_recv.at[c, src]).wait_recv()

        def hidden(i, carry, cols=cols):
            x = x_v[pl.ds(i * per_block, per_block)].reshape(block, dim)
            a = jnp.dot(x, w_v[0, :, cols], preferred_element_type=jnp.float32)
            b = jnp.dot(x, w_v[1, :, cols], preferred_element_type=jnp.float32)
            h_v[aligned(i, block, block), cols] = (a * jax.nn.sigmoid(a) * b).astype(jnp.bfloat16)
            return carry

        lax.fori_loop(0, ROW_BLOCKS, hidden, 0)
        if c == CHUNKS // 2:
            receive_next()

    def finish(g, between):
        if n_rep > 1:
            for q in range(DOWN_SPLIT):
                for src in reversed(peers):
                    down_pass(g, q, src, 1 - rep).wait_recv()

        def send_back(i):
            for j in range(per_block):
                s = i * per_block + j

                @pl.when(s != me)
                def _():
                    back_copy(g, s, me).start()

        def rows_out(n, carry):
            i = lax.rem(ep + n, ROW_BLOCKS)
            total = lax.dot_general(h_v[aligned(i, block, block), :], wd_v[g][...], (((1,), (1,)), ((), ())),
                                    preferred_element_type=jnp.float32)
            o_v[g][pl.ds(i * per_block, per_block)] = total.astype(jnp.bfloat16).reshape(
                per_block, cap, n_z * group_rows[g][1])

            @pl.when(n > 0)
            def _():
                send_back(lax.rem(i + ROW_BLOCKS - 1, ROW_BLOCKS))

            return carry

        lax.fori_loop(0, ROW_BLOCKS // 2, rows_out, 0)
        if between:
            receive_next()
        lax.fori_loop(ROW_BLOCKS // 2, ROW_BLOCKS, rows_out, 0)
        back_v[g][me] = o_v[g][me]
        send_back(lax.rem(ep + ROW_BLOCKS - 1, ROW_BLOCKS))

    for _ in range(DOWN_SPLIT - 1):
        receive_next()
    finish(0, True)
    for _ in range(DOWN_SPLIT - 1):
        receive_next()
    finish(1, False)

    every = pl.ds(0, ffn)
    for p in range(n_z - 1):
        for k in range(2):
            gate_up_copy(k, p, every, grecv.at[0, k, z]).wait_send()
        for g in range(2):
            for q in range(DOWN_SPLIT):
                down_copy(g, q, p).wait_send()
        if n_rep > 1:
            gate_up_pass(peers[p], rep, every, gpass_recv.at[0, peers[p]]).wait_send()
            for g in range(2):
                for q in range(DOWN_SPLIT):
                    down_pass(g, q, peers[p], rep).wait_send()

    scale = jnp.transpose(jnp.broadcast_to(gate_ref[...], (LANE, tok_count)))
    low_lanes = lax.broadcasted_iota(jnp.int32, (tok_count, LANE), 1) < HALF
    mixed = []

    def piece(half):
        src, j = divmod(half, part // HALF)
        g, start = (0, src * LANE) if j < 2 else (1, (src // 2) * LANE)
        return mixed[g][:, start:start + LANE], j if j < 2 else src % 2

    def put(t):
        (low, low_at), (high, high_at) = piece(2 * t), piece(2 * t + 1)
        low = low if low_at == 0 else pltpu.roll(low, HALF, 1)
        high = high if high_at == 1 else pltpu.roll(high, HALF, 1)
        cols = slice(t * LANE, (t + 1) * LANE)
        value = jnp.where(low_lanes, low, high)
        out_ref[:, cols] = (tok_v[:, cols].astype(jnp.float32) + scale * value).astype(jnp.bfloat16)

    only_first = [t for t in range(dim // LANE) if (2 * t) % 3 < 2 and (2 * t + 1) % 3 < 2]
    for g in range(2):
        for_others(lambda s, g=g: back_copy(g, s, s).wait())
        mixed.append(jnp.dot(sel_v[...], back_v[g][...].reshape(slots, n_z * group_rows[g][1]),
                             preferred_element_type=jnp.float32))
        for t in range(dim // LANE):
            if (t in only_first) == (g == 0):
                put(t)


def solution(mesh):
    n_rep, n_ep, n_z = mesh.shape["rep"], mesh.shape["ep"], mesh.shape["fsdp"]
    row_spec = P(("rep", "ep", "fsdp"), None)

    def device_step(tokens, expert_idx, gates, w_gate, w_up, w_down):
        tok_count, top_k = expert_idx.shape
        n_local, part, ffn = w_gate.shape
        dim = tokens.shape[1]
        assert top_k == 1 and n_local == n_z and n_ep == ROW_BLOCKS and part == LANE + HALF and n_rep <= 2
        n_dev = n_ep * n_z
        cap = (2 * tok_count + n_dev - 1) // n_dev
        slots = n_dev * cap
        any_spec = pl.BlockSpec(memory_space=pl.ANY)
        vmem_spec = pl.BlockSpec(memory_space=pltpu.VMEM)
        dma, bf16 = pltpu.SemaphoreType.DMA, jnp.bfloat16
        return pl.pallas_call(
            functools.partial(moe_kernel, n_rep, n_ep, n_z, cap),
            out_shape=jax.ShapeDtypeStruct((tok_count, dim), bf16),
            in_specs=[vmem_spec, vmem_spec, any_spec, any_spec, any_spec, any_spec],
            out_specs=vmem_spec,
            scratch_shapes=[
                pltpu.VMEM((tok_count, dim), bf16),
                pltpu.VMEM((n_dev, cap, dim), bf16),
                pltpu.VMEM((n_dev, cap, dim), bf16),
                pltpu.VMEM((2, n_z * part, ffn), bf16),
                pltpu.VMEM((n_z * LANE, ffn), bf16),
                pltpu.VMEM((n_z * HALF, ffn), bf16),
                pltpu.VMEM((slots, ffn), bf16),
                pltpu.VMEM((n_dev, cap, n_z * LANE), bf16),
                pltpu.VMEM((n_dev, cap, n_z * HALF), bf16),
                pltpu.VMEM((n_dev, cap, n_z * LANE), bf16),
                pltpu.VMEM((n_dev, cap, n_z * HALF), bf16),
                pltpu.VMEM((tok_count, slots), bf16),
                dma, dma((4,)),
                dma((2, n_z - 1)), dma((CHUNKS, 2, n_z)), dma((n_z,)), dma((CHUNKS, n_z)),
                dma((2, DOWN_SPLIT, n_z - 1)), dma((2, DOWN_SPLIT, n_z)), dma((2, DOWN_SPLIT, n_z)), dma((2, DOWN_SPLIT, n_z)),
                dma((n_dev,)), dma((n_dev,)), dma((2, n_dev)), dma((2, n_dev)),
            ],
            compiler_params=pltpu.CompilerParams(
                collective_id=0, has_side_effects=True, vmem_limit_bytes=60 * 1024 * 1024),
            cost_estimate=pl.CostEstimate(
                flops=6 * slots * dim * ffn, bytes_accessed=6 * dim * ffn, transcendentals=slots * ffn),
        )(expert_idx.reshape(1, tok_count), gates.reshape(1, tok_count), tokens, w_gate, w_up, jnp.swapaxes(w_down, 1, 2))

    return jax.shard_map(
        device_step, mesh=mesh,
        in_specs=(row_spec, row_spec, row_spec, P("ep", "fsdp", None), P("ep", "fsdp", None), P("ep", None, "fsdp")),
        out_specs=row_spec, check_vma=False)
```

```python
import functools

import jax
import jax.numpy as jnp
from jax import lax
from jax.experimental import pallas as pl
from jax.experimental.pallas import tpu as pltpu
from jax.sharding import PartitionSpec as P

MESH = pl.DeviceIdType.MESH
LANE = 128
HALF = 64
CHUNKS = 6
AHEAD = 4
ROWS_AFTER = 3
DOWN_SPLIT = 3
ROW_BLOCKS = 4


def aligned(start, size, step):
    return pl.ds(pl.multiple_of(start * step, step), size)


def moe_kernel(n_rep, n_ep, n_z, cap, idx_ref, gate_ref, tok_ref, wg_ref, wu_ref, wd_ref, out_ref,
               idx_v, gate_v, tok_v, out_v, send_v, x_v, w_v, wd0_v, wd1_v, h_v, o0_v, o1_v, back0_v, back1_v, sel_v,
               tok_sem, own_sem, gsend, grecv, gpass_send, gpass_recv, dsend, drecv, dpass_send, dpass_recv,
               xsend, xrecv, bsend, brecv, out_sem):
    rep, ep, z = lax.axis_index("rep"), lax.axis_index("ep"), lax.axis_index("fsdp")
    rep = rep if n_rep > 1 else 0
    me = ep * n_z + z
    n_dev = n_ep * n_z
    part, ffn = wg_ref.shape[1], wg_ref.shape[2]
    share, span = part // n_rep, ffn // n_rep // DOWN_SPLIT
    width = ffn // CHUNKS
    tok_count, dim = tok_ref.shape
    slots = n_dev * cap
    block, per_block = slots // ROW_BLOCKS, n_dev // ROW_BLOCKS
    gate_up = (wg_ref, wu_ref)
    wd_v, o_v, back_v = (wd0_v, wd1_v), (o0_v, o1_v), (back0_v, back1_v)
    group_rows = ((0, LANE), (LANE, HALF))
    other_rep = {"rep": lax.rem(rep + 1, n_rep)}

    def place(s):
        return {"ep": lax.div(s, n_z), "fsdp": lax.rem(s, n_z)}

    def remote(src, dst, send_sem, recv_sem, where):
        return pltpu.make_async_remote_copy(
            src_ref=src, dst_ref=dst, send_sem=send_sem, recv_sem=recv_sem, device_id=where, device_id_type=MESH)

    small = [pltpu.make_async_copy(ref, to, tok_sem.at[n])
             for n, (ref, to) in enumerate(((idx_ref, idx_v), (gate_ref, gate_v), (tok_ref, tok_v)))]
    own = []
    for k in range(2):
        own.append(pltpu.make_async_copy(gate_up[k].at[z], w_v.at[k, aligned(z, part, part), :], own_sem.at[k]))
    for g, (first, rows) in enumerate(group_rows):
        own.append(pltpu.make_async_copy(
            wd_ref.at[z, first:first + rows, :], wd_v[g].at[aligned(z, rows, rows), :], own_sem.at[2 + g]))
    for copy in small + own:
        copy.start()

    barrier = pltpu.get_barrier_semaphore()
    for d in range(1, n_dev):
        pl.semaphore_signal(barrier, inc=1, device_id=place(lax.rem(me + d, n_dev)), device_id_type=MESH)
    if n_rep > 1:
        pl.semaphore_signal(barrier, inc=1, device_id=other_rep, device_id_type=MESH)
    pl.semaphore_wait(barrier, n_dev - 1 + n_rep - 1)

    peers = [lax.rem(z + d, n_z) for d in range(1, n_z)]

    def share_rows(src, of_rep):
        return pl.ds(pl.multiple_of(src * part + of_rep * share, share), share)

    def gate_up_copy(k, p, cols, sem):
        zp = peers[p]
        return remote(gate_up[k].at[zp, aligned(rep, share, share), cols], w_v.at[k, share_rows(z, rep), cols],
                      gsend.at[k, p], sem, {"fsdp": zp})

    def gate_up_pass(src, of_rep, cols, sem):
        at = w_v.at[:, share_rows(src, of_rep), cols]
        return remote(at, at, gpass_send.at[src], sem, other_rep)

    def down_cols(of_rep, q):
        return aligned(of_rep * DOWN_SPLIT + q, span, span)

    def down_copy(g, q, p):
        zp = peers[p]
        first, rows = group_rows[g]
        cols = down_cols(rep, q)
        return remote(wd_ref.at[zp, first:first + rows, cols], wd_v[g].at[aligned(z, rows, rows), cols],
                      dsend.at[g, q, p], drecv.at[g, q, z], {"fsdp": zp})

    def down_pass(g, q, src, of_rep):
        rows = group_rows[g][1]
        at = wd_v[g].at[aligned(src, rows, rows), down_cols(of_rep, q)]
        return remote(at, at, dpass_send.at[g, q, src], dpass_recv.at[g, q, src], other_rep)

    def row_copy(s, at):
        return remote(send_v.at[s], x_v.at[at], xsend.at[s], xrecv.at[at], place(s))

    def back_copy(g, s, at):
        return remote(o_v[g].at[s], back_v[g].at[at], bsend.at[g, s], brecv.at[g, at], place(s))

    def for_others(run):
        def step(d, carry):
            run(lax.rem(me + d, n_dev))
            return carry
        lax.fori_loop(1, n_dev, step, 0)

    def send(item):
        if item < CHUNKS:
            cols = pl.ds(item * width, width)
            for p in range(n_z - 1):
                for k in range(2):
                    gate_up_copy(k, p, cols, grecv.at[item, k, z]).start()
        elif item == CHUNKS:
            for_others(lambda s: row_copy(s, me).start())
        elif item <= CHUNKS + 2 * DOWN_SPLIT:
            g, q = divmod(item - CHUNKS - 1, DOWN_SPLIT)
            for p in range(n_z - 1):
                down_copy(g, q, p).start()

    def receive(item):
        if item < CHUNKS:
            cols = pl.ds(item * width, width)
            for src in reversed(peers):
                for k in range(2):
                    at = w_v.at[k, share_rows(src, rep), cols]
                    remote(at, at, gsend.at[k, 0], grecv.at[item, k, src], {"fsdp": src}).wait_recv()
                if n_rep > 1:
                    gate_up_pass(src, rep, cols, gpass_recv.at[item, src]).start()
        elif item == CHUNKS:
            for_others(lambda s: row_copy(s, s).wait())
        else:
            g, q = divmod(item - CHUNKS - 1, DOWN_SPLIT)
            for src in reversed(peers):
                rows = group_rows[g][1]
                at = wd_v[g].at[aligned(src, rows, rows), down_cols(rep, q)]
                remote(at, at, dsend.at[g, q, 0], drecv.at[g, q, src], {"fsdp": src}).wait_recv()
                if n_rep > 1:
                    down_pass(g, q, src, rep).start()

    def make_rows():
        small[0].wait()
        small[1].wait()
        ids = idx_v[...]
        onehot = (lax.broadcasted_iota(jnp.int32, (n_dev, tok_count), 0) == ids).astype(jnp.float32)
        earlier = (lax.broadcasted_iota(jnp.int32, (tok_count, tok_count), 0)
                   < lax.broadcasted_iota(jnp.int32, (tok_count, tok_count), 1)).astype(jnp.bfloat16)
        before = jnp.dot(onehot.astype(jnp.bfloat16), earlier, preferred_element_type=jnp.float32)
        slot = jnp.sum(before * onehot, axis=0, keepdims=True)
        target = jnp.where(slot < cap, ids.astype(jnp.float32) * cap + slot, -1.0)

        small[2].wait()

        def dispatch(i, carry):
            want = lax.broadcasted_iota(jnp.int32, (block, tok_count), 0) + i * block
            pick = (want.astype(jnp.float32) == target).astype(jnp.bfloat16)
            picked = jnp.dot(pick, tok_v[...], preferred_element_type=jnp.float32).astype(jnp.bfloat16)
            send_v[pl.ds(i * per_block, per_block)] = picked.reshape(per_block, cap, dim)
            return carry

        lax.fori_loop(0, ROW_BLOCKS, dispatch, 0)
        x_v[me] = send_v[me]

        spread = jnp.transpose(jnp.broadcast_to(target, (LANE, tok_count)))
        for j in range(slots // LANE):
            want = lax.broadcasted_iota(jnp.int32, (tok_count, LANE), 1) + j * LANE
            sel_v[:, j * LANE:(j + 1) * LANE] = (spread == want.astype(jnp.float32)).astype(jnp.bfloat16)

    order = list(range(CHUNKS))
    order = order[:ROWS_AFTER] + [CHUNKS] + order[ROWS_AFTER:] + [CHUNKS + 1 + i for i in range(2 * DOWN_SPLIT)]
    for item in order[:AHEAD]:
        if item == CHUNKS:
            make_rows()
        send(item)
    if CHUNKS not in order[:AHEAD]:
        make_rows()

    at_item = iter(range(len(order)))

    def receive_next():
        n = next(at_item)
        receive(order[n])
        if n + AHEAD < len(order):
            send(order[n + AHEAD])

    for _ in range(ROWS_AFTER + 1):
        receive_next()

    for copy in own:
        copy.wait()
    for c in range(CHUNKS):
        cols = slice(c * width, (c + 1) * width)
        if n_rep > 1:
            for src in peers:
                gate_up_pass(src, 1 - rep, pl.ds(c * width, width), gpass_recv.at[c, src]).wait_recv()

        def hidden(i, carry, cols=cols):
            x = x_v[pl.ds(i * per_block, per_block)].reshape(block, dim)
            a = jnp.dot(x, w_v[0, :, cols], preferred_element_type=jnp.float32)
            b = jnp.dot(x, w_v[1, :, cols], preferred_element_type=jnp.float32)
            h_v[aligned(i, block, block), cols] = (a * jax.nn.sigmoid(a) * b).astype(jnp.bfloat16)
            return carry

        lax.fori_loop(0, ROW_BLOCKS, hidden, 0)
        if c > 0:
            receive_next()

    def finish(g, between):
        if n_rep > 1:
            for q in range(DOWN_SPLIT):
                for src in reversed(peers):
                    down_pass(g, q, src, 1 - rep).wait_recv()

        def send_back(i):
            for j in range(per_block):
                s = i * per_block + j

                @pl.when(s != me)
                def _():
                    back_copy(g, s, me).start()

        def rows_out(n, carry):
            i = lax.rem(ep + n, ROW_BLOCKS)
            total = lax.dot_general(h_v[aligned(i, block, block), :], wd_v[g][...], (((1,), (1,)), ((), ())),
                                    preferred_element_type=jnp.float32)
            o_v[g][pl.ds(i * per_block, per_block)] = total.astype(jnp.bfloat16).reshape(
                per_block, cap, n_z * group_rows[g][1])

            @pl.when(n > 0)
            def _():
                send_back(lax.rem(i + ROW_BLOCKS - 1, ROW_BLOCKS))

            return carry

        lax.fori_loop(0, ROW_BLOCKS // 2, rows_out, 0)
        if between:
            receive_next()
        lax.fori_loop(ROW_BLOCKS // 2, ROW_BLOCKS, rows_out, 0)
        back_v[g][me] = o_v[g][me]
        send_back(lax.rem(ep + ROW_BLOCKS - 1, ROW_BLOCKS))

    for _ in range(len(order) - (ROWS_AFTER + 1) - (CHUNKS - 1) - DOWN_SPLIT):
        receive_next()
    finish(0, True)
    for _ in range(DOWN_SPLIT - 1):
        receive_next()
    finish(1, False)

    every = pl.ds(0, ffn)
    for p in range(n_z - 1):
        for k in range(2):
            gate_up_copy(k, p, every, grecv.at[0, k, z]).wait_send()
        for g in range(2):
            for q in range(DOWN_SPLIT):
                down_copy(g, q, p).wait_send()
        if n_rep > 1:
            gate_up_pass(peers[p], rep, every, gpass_recv.at[0, peers[p]]).wait_send()
            for g in range(2):
                for q in range(DOWN_SPLIT):
                    down_pass(g, q, peers[p], rep).wait_send()

    scale = jnp.transpose(jnp.broadcast_to(gate_v[...], (LANE, tok_count)))
    low_lanes = lax.broadcasted_iota(jnp.int32, (tok_count, LANE), 1) < HALF
    mixed = []

    def piece(half):
        src, j = divmod(half, part // HALF)
        g, start = (0, src * LANE) if j < 2 else (1, (src // 2) * LANE)
        return mixed[g][:, start:start + LANE], j if j < 2 else src % 2

    def put(t):
        (low, low_at), (high, high_at) = piece(2 * t), piece(2 * t + 1)
        low = low if low_at == 0 else pltpu.roll(low, HALF, 1)
        high = high if high_at == 1 else pltpu.roll(high, HALF, 1)
        cols = slice(t * LANE, (t + 1) * LANE)
        value = jnp.where(low_lanes, low, high)
        out_v[t] = (tok_v[:, cols].astype(jnp.float32) + scale * value).astype(jnp.bfloat16)

    def store(t):
        return pltpu.make_async_copy(out_v.at[t], out_ref.at[:, t * LANE:(t + 1) * LANE], out_sem.at[t])

    only_first = [t for t in range(dim // LANE) if (2 * t) % 3 < 2 and (2 * t + 1) % 3 < 2]
    for g in range(2):
        for_others(lambda s, g=g: back_copy(g, s, s).wait())
        mixed.append(jnp.dot(sel_v[...], back_v[g][...].reshape(slots, n_z * group_rows[g][1]),
                             preferred_element_type=jnp.float32))
        for t in range(dim // LANE):
            if (t in only_first) == (g == 0):
                put(t)
        if g == 1:
            for t in range(dim // LANE):
                store(t).start()
    for t in range(dim // LANE):
        store(t).wait()


def solution(mesh):
    n_rep, n_ep, n_z = mesh.shape["rep"], mesh.shape["ep"], mesh.shape["fsdp"]
    row_spec = P(("rep", "ep", "fsdp"), None)

    def device_step(tokens, expert_idx, gates, w_gate, w_up, w_down):
        tok_count, top_k = expert_idx.shape
        n_local, part, ffn = w_gate.shape
        dim = tokens.shape[1]
        assert top_k == 1 and n_local == n_z and n_ep == ROW_BLOCKS and part == LANE + HALF and n_rep <= 2
        n_dev = n_ep * n_z
        cap = (2 * tok_count + n_dev - 1) // n_dev
        slots = n_dev * cap
        any_spec = pl.BlockSpec(memory_space=pl.ANY)
        dma, bf16 = pltpu.SemaphoreType.DMA, jnp.bfloat16
        return pl.pallas_call(
            functools.partial(moe_kernel, n_rep, n_ep, n_z, cap),
            out_shape=jax.ShapeDtypeStruct((tok_count, dim), bf16),
            in_specs=[any_spec, any_spec, any_spec, any_spec, any_spec, any_spec],
            out_specs=any_spec,
            scratch_shapes=[
                pltpu.VMEM((1, tok_count), jnp.int32),
                pltpu.VMEM((1, tok_count), jnp.float32),
                pltpu.VMEM((tok_count, dim), bf16),
                pltpu.VMEM((dim // LANE, tok_count, LANE), bf16),
                pltpu.VMEM((n_dev, cap, dim), bf16),
                pltpu.VMEM((n_dev, cap, dim), bf16),
                pltpu.VMEM((2, n_z * part, ffn), bf16),
                pltpu.VMEM((n_z * LANE, ffn), bf16),
                pltpu.VMEM((n_z * HALF, ffn), bf16),
                pltpu.VMEM((slots, ffn), bf16),
                pltpu.VMEM((n_dev, cap, n_z * LANE), bf16),
                pltpu.VMEM((n_dev, cap, n_z * HALF), bf16),
                pltpu.VMEM((n_dev, cap, n_z * LANE), bf16),
                pltpu.VMEM((n_dev, cap, n_z * HALF), bf16),
                pltpu.VMEM((tok_count, slots), bf16),
                dma((3,)), dma((4,)),
                dma((2, n_z - 1)), dma((CHUNKS, 2, n_z)), dma((n_z,)), dma((CHUNKS, n_z)),
                dma((2, DOWN_SPLIT, n_z - 1)), dma((2, DOWN_SPLIT, n_z)), dma((2, DOWN_SPLIT, n_z)), dma((2, DOWN_SPLIT, n_z)),
                dma((n_dev,)), dma((n_dev,)), dma((2, n_dev)), dma((2, n_dev)), dma((dim // LANE,)),
            ],
            compiler_params=pltpu.CompilerParams(
                collective_id=0, has_side_effects=True, vmem_limit_bytes=60 * 1024 * 1024),
            cost_estimate=pl.CostEstimate(
                flops=6 * slots * dim * ffn, bytes_accessed=6 * dim * ffn, transcendentals=slots * ffn),
        )(expert_idx.reshape(1, tok_count), gates.reshape(1, tok_count), tokens, w_gate, w_up, jnp.swapaxes(w_down, 1, 2))

    return jax.shard_map(
        device_step, mesh=mesh,
        in_specs=(row_spec, row_spec, row_spec, P("ep", "fsdp", None), P("ep", "fsdp", None), P("ep", None, "fsdp")),
        out_specs=row_spec, check_vma=False)
```

```python
import functools

import jax
import jax.numpy as jnp
from jax import lax
from jax.experimental import pallas as pl
from jax.experimental.pallas import tpu as pltpu
from jax.sharding import PartitionSpec as P

MESH = pl.DeviceIdType.MESH
LANE = 128
HALF = 64
CHUNKS = 6
AHEAD = 3
ROWS_AFTER = 6
STEPS = "RRRRRRR HHHH R HH RR F R f RR Ff"
DOWN_SPLIT = 3
ROW_BLOCKS = 4


def aligned(start, size, step):
    return pl.ds(pl.multiple_of(start * step, step), size)


def moe_kernel(n_rep, n_ep, n_z, cap, idx_ref, gate_ref, tok_ref, wg_ref, wu_ref, wd_ref, out_ref,
               idx_v, gate_v, tok_v, out_v, send_v, x_v, w_v, wd0_v, wd1_v, h_v, o0_v, o1_v, back0_v, back1_v, sel_v,
               tok_sem, own_sem, gsend, grecv, gpass_send, gpass_recv, dsend, drecv, dpass_send, dpass_recv,
               xsend, xrecv, bsend, brecv, out_sem):
    rep, ep, z = lax.axis_index("rep"), lax.axis_index("ep"), lax.axis_index("fsdp")
    rep = rep if n_rep > 1 else 0
    me = ep * n_z + z
    n_dev = n_ep * n_z
    part, ffn = wg_ref.shape[1], wg_ref.shape[2]
    share, span = part // n_rep, ffn // n_rep // DOWN_SPLIT
    width = ffn // CHUNKS
    tok_count, dim = tok_ref.shape
    slots = n_dev * cap
    block, per_block = slots // ROW_BLOCKS, n_dev // ROW_BLOCKS
    gate_up = (wg_ref, wu_ref)
    wd_v, o_v, back_v = (wd0_v, wd1_v), (o0_v, o1_v), (back0_v, back1_v)
    group_rows = ((0, LANE), (LANE, HALF))
    other_rep = {"rep": lax.rem(rep + 1, n_rep)}

    def place(s):
        return {"ep": lax.div(s, n_z), "fsdp": lax.rem(s, n_z)}

    def remote(src, dst, send_sem, recv_sem, where):
        return pltpu.make_async_remote_copy(
            src_ref=src, dst_ref=dst, send_sem=send_sem, recv_sem=recv_sem, device_id=where, device_id_type=MESH)

    small = [pltpu.make_async_copy(ref, to, tok_sem.at[n])
             for n, (ref, to) in enumerate(((idx_ref, idx_v), (gate_ref, gate_v), (tok_ref, tok_v)))]
    own = []
    for k in range(2):
        own.append(pltpu.make_async_copy(gate_up[k].at[z], w_v.at[k, aligned(z, part, part), :], own_sem.at[k]))
    for g, (first, rows) in enumerate(group_rows):
        own.append(pltpu.make_async_copy(
            wd_ref.at[z, first:first + rows, :], wd_v[g].at[aligned(z, rows, rows), :], own_sem.at[2 + g]))
    for copy in small + own:
        copy.start()

    barrier = pltpu.get_barrier_semaphore()
    for d in range(1, n_dev):
        pl.semaphore_signal(barrier, inc=1, device_id=place(lax.rem(me + d, n_dev)), device_id_type=MESH)
    if n_rep > 1:
        pl.semaphore_signal(barrier, inc=1, device_id=other_rep, device_id_type=MESH)
    pl.semaphore_wait(barrier, n_dev - 1 + n_rep - 1)

    peers = [lax.rem(z + d, n_z) for d in range(1, n_z)]

    def share_rows(src, of_rep):
        return pl.ds(pl.multiple_of(src * part + of_rep * share, share), share)

    def gate_up_copy(k, p, cols, sem):
        zp = peers[p]
        return remote(gate_up[k].at[zp, aligned(rep, share, share), cols], w_v.at[k, share_rows(z, rep), cols],
                      gsend.at[k, p], sem, {"fsdp": zp})

    def gate_up_pass(src, of_rep, cols, sem):
        at = w_v.at[:, share_rows(src, of_rep), cols]
        return remote(at, at, gpass_send.at[src], sem, other_rep)

    def down_cols(of_rep, q):
        return aligned(of_rep * DOWN_SPLIT + q, span, span)

    def down_copy(g, q, p):
        zp = peers[p]
        first, rows = group_rows[g]
        cols = down_cols(rep, q)
        return remote(wd_ref.at[zp, first:first + rows, cols], wd_v[g].at[aligned(z, rows, rows), cols],
                      dsend.at[g, q, p], drecv.at[g, q, z], {"fsdp": zp})

    def down_pass(g, q, src, of_rep):
        rows = group_rows[g][1]
        at = wd_v[g].at[aligned(src, rows, rows), down_cols(of_rep, q)]
        return remote(at, at, dpass_send.at[g, q, src], dpass_recv.at[g, q, src], other_rep)

    def row_copy(s, at):
        return remote(send_v.at[s], x_v.at[at], xsend.at[s], xrecv.at[at], place(s))

    def back_copy(g, s, at):
        return remote(o_v[g].at[s], back_v[g].at[at], bsend.at[g, s], brecv.at[g, at], place(s))

    def for_others(run):
        def step(d, carry):
            run(lax.rem(me + d, n_dev))
            return carry
        lax.fori_loop(1, n_dev, step, 0)

    def send(item):
        if item < CHUNKS:
            cols = pl.ds(item * width, width)
            for p in range(n_z - 1):
                for k in range(2):
                    gate_up_copy(k, p, cols, grecv.at[item, k, z]).start()
        elif item == CHUNKS:
            for_others(lambda s: row_copy(s, me).start())
        elif item <= CHUNKS + 2 * DOWN_SPLIT:
            g, q = divmod(item - CHUNKS - 1, DOWN_SPLIT)
            for p in range(n_z - 1):
                down_copy(g, q, p).start()

    def receive(item):
        if item < CHUNKS:
            cols = pl.ds(item * width, width)
            for src in reversed(peers):
                for k in range(2):
                    at = w_v.at[k, share_rows(src, rep), cols]
                    remote(at, at, gsend.at[k, 0], grecv.at[item, k, src], {"fsdp": src}).wait_recv()
                if n_rep > 1:
                    gate_up_pass(src, rep, cols, gpass_recv.at[item, src]).start()
        elif item == CHUNKS:
            for_others(lambda s: row_copy(s, s).wait())
        else:
            g, q = divmod(item - CHUNKS - 1, DOWN_SPLIT)
            for src in reversed(peers):
                rows = group_rows[g][1]
                at = wd_v[g].at[aligned(src, rows, rows), down_cols(rep, q)]
                remote(at, at, dsend.at[g, q, 0], drecv.at[g, q, src], {"fsdp": src}).wait_recv()
                if n_rep > 1:
                    down_pass(g, q, src, rep).start()

    def make_rows():
        small[0].wait()
        small[1].wait()
        ids = idx_v[...]
        onehot = (lax.broadcasted_iota(jnp.int32, (n_dev, tok_count), 0) == ids).astype(jnp.float32)
        earlier = (lax.broadcasted_iota(jnp.int32, (tok_count, tok_count), 0)
                   < lax.broadcasted_iota(jnp.int32, (tok_count, tok_count), 1)).astype(jnp.bfloat16)
        before = jnp.dot(onehot.astype(jnp.bfloat16), earlier, preferred_element_type=jnp.float32)
        slot = jnp.sum(before * onehot, axis=0, keepdims=True)
        target = jnp.where(slot < cap, ids.astype(jnp.float32) * cap + slot, -1.0)

        small[2].wait()

        def dispatch(i, carry):
            want = lax.broadcasted_iota(jnp.int32, (block, tok_count), 0) + i * block
            pick = (want.astype(jnp.float32) == target).astype(jnp.bfloat16)
            picked = jnp.dot(pick, tok_v[...], preferred_element_type=jnp.float32).astype(jnp.bfloat16)
            send_v[pl.ds(i * per_block, per_block)] = picked.reshape(per_block, cap, dim)
            return carry

        lax.fori_loop(0, ROW_BLOCKS, dispatch, 0)
        x_v[me] = send_v[me]

        spread = jnp.transpose(jnp.broadcast_to(target, (LANE, tok_count)))
        for j in range(slots // LANE):
            want = lax.broadcasted_iota(jnp.int32, (tok_count, LANE), 1) + j * LANE
            sel_v[:, j * LANE:(j + 1) * LANE] = (spread == want.astype(jnp.float32)).astype(jnp.bfloat16)

    order = list(range(CHUNKS))
    order = order[:ROWS_AFTER] + [CHUNKS] + order[ROWS_AFTER:] + [CHUNKS + 1 + i for i in range(2 * DOWN_SPLIT)]
    for item in order[:AHEAD]:
        if item == CHUNKS:
            make_rows()
        send(item)
    if CHUNKS not in order[:AHEAD]:
        make_rows()

    at_item = iter(range(len(order)))

    def receive_next():
        n = next(at_item)
        receive(order[n])
        if n + AHEAD < len(order):
            send(order[n + AHEAD])

    def hidden_chunk(c):
        cols = slice(c * width, (c + 1) * width)
        if c == 0:
            for copy in own:
                copy.wait()
        if n_rep > 1:
            for src in peers:
                gate_up_pass(src, 1 - rep, pl.ds(c * width, width), gpass_recv.at[c, src]).wait_recv()

        def hidden(i, carry, cols=cols):
            x = x_v[pl.ds(i * per_block, per_block)].reshape(block, dim)
            a = jnp.dot(x, w_v[0, :, cols], preferred_element_type=jnp.float32)
            b = jnp.dot(x, w_v[1, :, cols], preferred_element_type=jnp.float32)
            h_v[aligned(i, block, block), cols] = (a * jax.nn.sigmoid(a) * b).astype(jnp.bfloat16)
            return carry

        lax.fori_loop(0, ROW_BLOCKS, hidden, 0)

    def finish(g, half):
        if n_rep > 1 and half == 0:
            for q in range(DOWN_SPLIT):
                for src in reversed(peers):
                    down_pass(g, q, src, 1 - rep).wait_recv()

        def send_back(i):
            for j in range(per_block):
                s = i * per_block + j

                @pl.when(s != me)
                def _():
                    back_copy(g, s, me).start()

        def rows_out(n, carry):
            i = lax.rem(ep + n, ROW_BLOCKS)
            total = lax.dot_general(h_v[aligned(i, block, block), :], wd_v[g][...], (((1,), (1,)), ((), ())),
                                    preferred_element_type=jnp.float32)
            o_v[g][pl.ds(i * per_block, per_block)] = total.astype(jnp.bfloat16).reshape(
                per_block, cap, n_z * group_rows[g][1])

            @pl.when(n > 0)
            def _():
                send_back(lax.rem(i + ROW_BLOCKS - 1, ROW_BLOCKS))

            return carry

        lax.fori_loop(half * ROW_BLOCKS // 2, (half + 1) * ROW_BLOCKS // 2, rows_out, 0)
        if half == 1:
            back_v[g][me] = o_v[g][me]
            send_back(lax.rem(ep + ROW_BLOCKS - 1, ROW_BLOCKS))

    chunk_count, group_count = iter(range(CHUNKS)), iter((0, 0, 1, 1))
    for step in STEPS.replace(" ", ""):
        if step == "R":
            receive_next()
        elif step == "H":
            hidden_chunk(next(chunk_count))
        else:
            finish(next(group_count), int(step == "f"))

    every = pl.ds(0, ffn)
    for p in range(n_z - 1):
        for k in range(2):
            gate_up_copy(k, p, every, grecv.at[0, k, z]).wait_send()
        for g in range(2):
            for q in range(DOWN_SPLIT):
                down_copy(g, q, p).wait_send()
        if n_rep > 1:
            gate_up_pass(peers[p], rep, every, gpass_recv.at[0, peers[p]]).wait_send()
            for g in range(2):
                for q in range(DOWN_SPLIT):
                    down_pass(g, q, peers[p], rep).wait_send()

    scale = jnp.transpose(jnp.broadcast_to(gate_v[...], (LANE, tok_count)))
    low_lanes = lax.broadcasted_iota(jnp.int32, (tok_count, LANE), 1) < HALF
    mixed = []

    def piece(half):
        src, j = divmod(half, part // HALF)
        g, start = (0, src * LANE) if j < 2 else (1, (src // 2) * LANE)
        return mixed[g][:, start:start + LANE], j if j < 2 else src % 2

    def put(t):
        (low, low_at), (high, high_at) = piece(2 * t), piece(2 * t + 1)
        low = low if low_at == 0 else pltpu.roll(low, HALF, 1)
        high = high if high_at == 1 else pltpu.roll(high, HALF, 1)
        cols = slice(t * LANE, (t + 1) * LANE)
        value = jnp.where(low_lanes, low, high)
        out_v[t] = (tok_v[:, cols].astype(jnp.float32) + scale * value).astype(jnp.bfloat16)

    def store(t):
        return pltpu.make_async_copy(out_v.at[t], out_ref.at[:, t * LANE:(t + 1) * LANE], out_sem.at[t])

    only_first = [t for t in range(dim // LANE) if (2 * t) % 3 < 2 and (2 * t + 1) % 3 < 2]
    for g in range(2):
        for_others(lambda s, g=g: back_copy(g, s, s).wait())
        mixed.append(jnp.dot(sel_v[...], back_v[g][...].reshape(slots, n_z * group_rows[g][1]),
                             preferred_element_type=jnp.float32))
        for t in range(dim // LANE):
            if (t in only_first) == (g == 0):
                put(t)
        if g == 1:
            for t in range(dim // LANE):
                store(t).start()
    for t in range(dim // LANE):
        store(t).wait()


def solution(mesh):
    n_rep, n_ep, n_z = mesh.shape["rep"], mesh.shape["ep"], mesh.shape["fsdp"]
    row_spec = P(("rep", "ep", "fsdp"), None)

    def device_step(tokens, expert_idx, gates, w_gate, w_up, w_down):
        tok_count, top_k = expert_idx.shape
        n_local, part, ffn = w_gate.shape
        dim = tokens.shape[1]
        assert top_k == 1 and n_local == n_z and n_ep == ROW_BLOCKS and part == LANE + HALF and n_rep <= 2
        n_dev = n_ep * n_z
        cap = (2 * tok_count + n_dev - 1) // n_dev
        slots = n_dev * cap
        any_spec = pl.BlockSpec(memory_space=pl.ANY)
        dma, bf16 = pltpu.SemaphoreType.DMA, jnp.bfloat16
        return pl.pallas_call(
            functools.partial(moe_kernel, n_rep, n_ep, n_z, cap),
            out_shape=jax.ShapeDtypeStruct((tok_count, dim), bf16),
            in_specs=[any_spec, any_spec, any_spec, any_spec, any_spec, any_spec],
            out_specs=any_spec,
            scratch_shapes=[
                pltpu.VMEM((1, tok_count), jnp.int32),
                pltpu.VMEM((1, tok_count), jnp.float32),
                pltpu.VMEM((tok_count, dim), bf16),
                pltpu.VMEM((dim // LANE, tok_count, LANE), bf16),
                pltpu.VMEM((n_dev, cap, dim), bf16),
                pltpu.VMEM((n_dev, cap, dim), bf16),
                pltpu.VMEM((2, n_z * part, ffn), bf16),
                pltpu.VMEM((n_z * LANE, ffn), bf16),
                pltpu.VMEM((n_z * HALF, ffn), bf16),
                pltpu.VMEM((slots, ffn), bf16),
                pltpu.VMEM((n_dev, cap, n_z * LANE), bf16),
                pltpu.VMEM((n_dev, cap, n_z * HALF), bf16),
                pltpu.VMEM((n_dev, cap, n_z * LANE), bf16),
                pltpu.VMEM((n_dev, cap, n_z * HALF), bf16),
                pltpu.VMEM((tok_count, slots), bf16),
                dma((3,)), dma((4,)),
                dma((2, n_z - 1)), dma((CHUNKS, 2, n_z)), dma((n_z,)), dma((CHUNKS, n_z)),
                dma((2, DOWN_SPLIT, n_z - 1)), dma((2, DOWN_SPLIT, n_z)), dma((2, DOWN_SPLIT, n_z)), dma((2, DOWN_SPLIT, n_z)),
                dma((n_dev,)), dma((n_dev,)), dma((2, n_dev)), dma((2, n_dev)), dma((dim // LANE,)),
            ],
            compiler_params=pltpu.CompilerParams(
                collective_id=0, has_side_effects=True, vmem_limit_bytes=60 * 1024 * 1024),
            cost_estimate=pl.CostEstimate(
                flops=6 * slots * dim * ffn, bytes_accessed=6 * dim * ffn, transcendentals=slots * ffn),
        )(expert_idx.reshape(1, tok_count), gates.reshape(1, tok_count), tokens, w_gate, w_up, jnp.swapaxes(w_down, 1, 2))

    return jax.shard_map(
        device_step, mesh=mesh,
        in_specs=(row_spec, row_spec, row_spec, P("ep", "fsdp", None), P("ep", "fsdp", None), P("ep", None, "fsdp")),
        out_specs=row_spec, check_vma=False)
```

```python
import functools

import jax
import jax.numpy as jnp
from jax import lax
from jax.experimental import pallas as pl
from jax.experimental.pallas import tpu as pltpu
from jax.sharding import PartitionSpec as P

MESH = pl.DeviceIdType.MESH
LANE = 128
HALF = 64
CHUNKS = 6
AHEAD = 4
ROWS_AFTER = 3
STEPS = "RRRR H HR HR HR HR HR R F R f RR Ff"
DOWN_SPLIT = 3
ROW_BLOCKS = 4


def aligned(start, size, step):
    return pl.ds(pl.multiple_of(start * step, step), size)


def moe_kernel(n_rep, n_ep, n_z, cap, idx_ref, gate_ref, tok_ref, wg_ref, wu_ref, wd_ref, out_ref,
               idx_v, gate_v, tok_v, out_v, send_v, x_v, w_v, wd0_v, wd1_v, h_v, o0_v, o1_v, back0_v, back1_v, sel_v,
               tok_sem, own_sem, gsend, grecv, gpass_send, gpass_recv, dsend, drecv, dpass_send, dpass_recv,
               xsend, xrecv, bsend, brecv, out_sem):
    rep, ep, z = lax.axis_index("rep"), lax.axis_index("ep"), lax.axis_index("fsdp")
    rep = rep if n_rep > 1 else 0
    me = ep * n_z + z
    n_dev = n_ep * n_z
    part, ffn = wg_ref.shape[1], wg_ref.shape[2]
    share, span = part // n_rep, ffn // n_rep // DOWN_SPLIT
    width = ffn // CHUNKS
    tok_count, dim = tok_ref.shape
    slots = n_dev * cap
    block, per_block = slots // ROW_BLOCKS, n_dev // ROW_BLOCKS
    gate_up = (wg_ref, wu_ref)
    wd_v, o_v, back_v = (wd0_v, wd1_v), (o0_v, o1_v), (back0_v, back1_v)
    group_rows = ((0, LANE), (LANE, HALF))
    other_rep = {"rep": lax.rem(rep + 1, n_rep)}

    def place(s):
        return {"ep": lax.div(s, n_z), "fsdp": lax.rem(s, n_z)}

    def remote(src, dst, send_sem, recv_sem, where):
        return pltpu.make_async_remote_copy(
            src_ref=src, dst_ref=dst, send_sem=send_sem, recv_sem=recv_sem, device_id=where, device_id_type=MESH)

    small = [pltpu.make_async_copy(ref, to, tok_sem.at[n])
             for n, (ref, to) in enumerate(((idx_ref, idx_v), (gate_ref, gate_v), (tok_ref, tok_v)))]
    own = []
    for k in range(2):
        own.append(pltpu.make_async_copy(gate_up[k].at[z], w_v.at[k, aligned(z, part, part), :], own_sem.at[k]))
    for g, (first, rows) in enumerate(group_rows):
        own.append(pltpu.make_async_copy(
            wd_ref.at[z, first:first + rows, :], wd_v[g].at[aligned(z, rows, rows), :], own_sem.at[2 + g]))
    for copy in small + own:
        copy.start()

    barrier = pltpu.get_barrier_semaphore()
    for d in range(1, n_dev):
        pl.semaphore_signal(barrier, inc=1, device_id=place(lax.rem(me + d, n_dev)), device_id_type=MESH)
    if n_rep > 1:
        pl.semaphore_signal(barrier, inc=1, device_id=other_rep, device_id_type=MESH)
    pl.semaphore_wait(barrier, n_dev - 1 + n_rep - 1)

    flip = lax.div(z, n_z // 2)

    def mirror(t):
        return t + flip * (n_z - 1 - 2 * t)

    peers = [mirror(t) for t in [1 - mirror(z)] + list(range(n_z // 2, n_z))]

    def share_rows(src, of_rep):
        return pl.ds(pl.multiple_of(src * part + of_rep * share, share), share)

    def gate_up_copy(k, p, cols, sem):
        zp = peers[p]
        return remote(gate_up[k].at[zp, aligned(rep, share, share), cols], w_v.at[k, share_rows(z, rep), cols],
                      gsend.at[k, p], sem, {"fsdp": zp})

    def gate_up_pass(src, of_rep, cols, sem):
        at = w_v.at[:, share_rows(src, of_rep), cols]
        return remote(at, at, gpass_send.at[src], sem, other_rep)

    def down_cols(of_rep, q):
        return aligned(of_rep * DOWN_SPLIT + q, span, span)

    def down_copy(g, q, p):
        zp = peers[p]
        first, rows = group_rows[g]
        cols = down_cols(rep, q)
        return remote(wd_ref.at[zp, first:first + rows, cols], wd_v[g].at[aligned(z, rows, rows), cols],
                      dsend.at[g, q, p], drecv.at[g, q, z], {"fsdp": zp})

    def down_pass(g, q, src, of_rep):
        rows = group_rows[g][1]
        at = wd_v[g].at[aligned(src, rows, rows), down_cols(of_rep, q)]
        return remote(at, at, dpass_send.at[g, q, src], dpass_recv.at[g, q, src], other_rep)

    def row_copy(s, at):
        return remote(send_v.at[s], x_v.at[at], xsend.at[s], xrecv.at[at], place(s))

    def back_copy(g, s, at):
        return remote(o_v[g].at[s], back_v[g].at[at], bsend.at[g, s], brecv.at[g, at], place(s))

    def for_others(run):
        def step(d, carry):
            first = lax.rem(ep + d, n_ep) * n_z

            @pl.when(d > 0)
            def _():
                run(first + z)

            for p in peers:
                run(first + p)
            return carry
        lax.fori_loop(0, n_ep, step, 0)

    def send(item):
        if item < CHUNKS:
            cols = pl.ds(item * width, width)
            for p in range(n_z - 1):
                for k in range(2):
                    gate_up_copy(k, p, cols, grecv.at[item, k, z]).start()
        elif item == CHUNKS:
            for_others(lambda s: row_copy(s, me).start())
        elif item <= CHUNKS + 2 * DOWN_SPLIT:
            g, q = divmod(item - CHUNKS - 1, DOWN_SPLIT)
            for p in range(n_z - 1):
                down_copy(g, q, p).start()

    def receive(item):
        if item < CHUNKS:
            cols = pl.ds(item * width, width)
            for src in peers:
                for k in range(2):
                    at = w_v.at[k, share_rows(src, rep), cols]
                    remote(at, at, gsend.at[k, 0], grecv.at[item, k, src], {"fsdp": src}).wait_recv()
                if n_rep > 1:
                    gate_up_pass(src, rep, cols, gpass_recv.at[item, src]).start()
        elif item == CHUNKS:
            for_others(lambda s: row_copy(s, s).wait())
        else:
            g, q = divmod(item - CHUNKS - 1, DOWN_SPLIT)
            for src in peers:
                rows = group_rows[g][1]
                at = wd_v[g].at[aligned(src, rows, rows), down_cols(rep, q)]
                remote(at, at, dsend.at[g, q, 0], drecv.at[g, q, src], {"fsdp": src}).wait_recv()
                if n_rep > 1:
                    down_pass(g, q, src, rep).start()

    def make_rows():
        small[0].wait()
        small[1].wait()
        ids = idx_v[...]
        onehot = (lax.broadcasted_iota(jnp.int32, (n_dev, tok_count), 0) == ids).astype(jnp.float32)
        earlier = (lax.broadcasted_iota(jnp.int32, (tok_count, tok_count), 0)
                   < lax.broadcasted_iota(jnp.int32, (tok_count, tok_count), 1)).astype(jnp.bfloat16)
        before = jnp.dot(onehot.astype(jnp.bfloat16), earlier, preferred_element_type=jnp.float32)
        slot = jnp.sum(before * onehot, axis=0, keepdims=True)
        target = jnp.where(slot < cap, ids.astype(jnp.float32) * cap + slot, -1.0)

        small[2].wait()

        def dispatch(i, carry):
            want = lax.broadcasted_iota(jnp.int32, (block, tok_count), 0) + i * block
            pick = (want.astype(jnp.float32) == target).astype(jnp.bfloat16)
            picked = jnp.dot(pick, tok_v[...], preferred_element_type=jnp.float32).astype(jnp.bfloat16)
            send_v[pl.ds(i * per_block, per_block)] = picked.reshape(per_block, cap, dim)
            return carry

        lax.fori_loop(0, ROW_BLOCKS, dispatch, 0)
        x_v[me] = send_v[me]

        spread = jnp.transpose(jnp.broadcast_to(target, (LANE, tok_count)))
        for j in range(slots // LANE):
            want = lax.broadcasted_iota(jnp.int32, (tok_count, LANE), 1) + j * LANE
            sel_v[:, j * LANE:(j + 1) * LANE] = (spread == want.astype(jnp.float32)).astype(jnp.bfloat16)

    order = list(range(CHUNKS))
    order = order[:ROWS_AFTER] + [CHUNKS] + order[ROWS_AFTER:] + [CHUNKS + 1 + i for i in range(2 * DOWN_SPLIT)]
    for item in order[:AHEAD]:
        if item == CHUNKS:
            make_rows()
        send(item)
    if CHUNKS not in order[:AHEAD]:
        make_rows()

    at_item = iter(range(len(order)))

    def receive_next():
        n = next(at_item)
        receive(order[n])
        if n + AHEAD < len(order):
            send(order[n + AHEAD])

    def hidden_chunk(c):
        cols = slice(c * width, (c + 1) * width)
        if c == 0:
            for copy in own:
                copy.wait()
        if n_rep > 1:
            for src in peers:
                gate_up_pass(src, 1 - rep, pl.ds(c * width, width), gpass_recv.at[c, src]).wait_recv()

        def hidden(i, carry, cols=cols):
            x = x_v[pl.ds(i * per_block, per_block)].reshape(block, dim)
            a = jnp.dot(x, w_v[0, :, cols], preferred_element_type=jnp.float32)
            b = jnp.dot(x, w_v[1, :, cols], preferred_element_type=jnp.float32)
            h_v[aligned(i, block, block), cols] = (a * jax.nn.sigmoid(a) * b).astype(jnp.bfloat16)
            return carry

        lax.fori_loop(0, ROW_BLOCKS, hidden, 0)

    def finish(g, half):
        if n_rep > 1 and half == 0:
            for q in range(DOWN_SPLIT):
                for src in peers:
                    down_pass(g, q, src, 1 - rep).wait_recv()

        def send_back(i):
            for p in peers:
                back_copy(g, i * per_block + p, me).start()

            @pl.when(i != ep)
            def _():
                back_copy(g, i * per_block + z, me).start()

        def rows_out(n, carry):
            i = lax.rem(ep + n, ROW_BLOCKS)
            total = lax.dot_general(h_v[aligned(i, block, block), :], wd_v[g][...], (((1,), (1,)), ((), ())),
                                    preferred_element_type=jnp.float32)
            o_v[g][pl.ds(i * per_block, per_block)] = total.astype(jnp.bfloat16).reshape(
                per_block, cap, n_z * group_rows[g][1])

            @pl.when(n > 0)
            def _():
                send_back(lax.rem(i + ROW_BLOCKS - 1, ROW_BLOCKS))

            return carry

        lax.fori_loop(half * ROW_BLOCKS // 2, (half + 1) * ROW_BLOCKS // 2, rows_out, 0)
        if half == 1:
            back_v[g][me] = o_v[g][me]
            send_back(lax.rem(ep + ROW_BLOCKS - 1, ROW_BLOCKS))

    chunk_count, group_count = iter(range(CHUNKS)), iter((0, 0, 1, 1))
    for step in STEPS.replace(" ", ""):
        if step == "R":
            receive_next()
        elif step == "H":
            hidden_chunk(next(chunk_count))
        else:
            finish(next(group_count), int(step == "f"))

    every = pl.ds(0, ffn)
    for p in range(n_z - 1):
        for k in range(2):
            gate_up_copy(k, p, every, grecv.at[0, k, z]).wait_send()
        for g in range(2):
            for q in range(DOWN_SPLIT):
                down_copy(g, q, p).wait_send()
        if n_rep > 1:
            gate_up_pass(peers[p], rep, every, gpass_recv.at[0, peers[p]]).wait_send()
            for g in range(2):
                for q in range(DOWN_SPLIT):
                    down_pass(g, q, peers[p], rep).wait_send()

    scale = jnp.transpose(jnp.broadcast_to(gate_v[...], (LANE, tok_count)))
    low_lanes = lax.broadcasted_iota(jnp.int32, (tok_count, LANE), 1) < HALF
    mixed = []

    def piece(half):
        src, j = divmod(half, part // HALF)
        g, start = (0, src * LANE) if j < 2 else (1, (src // 2) * LANE)
        return mixed[g][:, start:start + LANE], j if j < 2 else src % 2

    def put(t):
        (low, low_at), (high, high_at) = piece(2 * t), piece(2 * t + 1)
        low = low if low_at == 0 else pltpu.roll(low, HALF, 1)
        high = high if high_at == 1 else pltpu.roll(high, HALF, 1)
        cols = slice(t * LANE, (t + 1) * LANE)
        value = jnp.where(low_lanes, low, high)
        out_v[t] = (tok_v[:, cols].astype(jnp.float32) + scale * value).astype(jnp.bfloat16)

    def store(t):
        return pltpu.make_async_copy(out_v.at[t], out_ref.at[:, t * LANE:(t + 1) * LANE], out_sem.at[t])

    only_first = [t for t in range(dim // LANE) if (2 * t) % 3 < 2 and (2 * t + 1) % 3 < 2]
    for g in range(2):
        for_others(lambda s, g=g: back_copy(g, s, s).wait())
        mixed.append(jnp.dot(sel_v[...], back_v[g][...].reshape(slots, n_z * group_rows[g][1]),
                             preferred_element_type=jnp.float32))
        for t in range(dim // LANE):
            if (t in only_first) == (g == 0):
                put(t)
        if g == 1:
            for t in range(dim // LANE):
                store(t).start()
    for t in range(dim // LANE):
        store(t).wait()


def solution(mesh):
    n_rep, n_ep, n_z = mesh.shape["rep"], mesh.shape["ep"], mesh.shape["fsdp"]
    row_spec = P(("rep", "ep", "fsdp"), None)

    def device_step(tokens, expert_idx, gates, w_gate, w_up, w_down):
        tok_count, top_k = expert_idx.shape
        n_local, part, ffn = w_gate.shape
        dim = tokens.shape[1]
        assert top_k == 1 and n_local == n_z and n_ep == ROW_BLOCKS and n_z == 4 and part == LANE + HALF and n_rep <= 2
        n_dev = n_ep * n_z
        cap = (2 * tok_count + n_dev - 1) // n_dev
        slots = n_dev * cap
        any_spec = pl.BlockSpec(memory_space=pl.ANY)
        dma, bf16 = pltpu.SemaphoreType.DMA, jnp.bfloat16
        return pl.pallas_call(
            functools.partial(moe_kernel, n_rep, n_ep, n_z, cap),
            out_shape=jax.ShapeDtypeStruct((tok_count, dim), bf16),
            in_specs=[any_spec, any_spec, any_spec, any_spec, any_spec, any_spec],
            out_specs=any_spec,
            scratch_shapes=[
                pltpu.VMEM((1, tok_count), jnp.int32),
                pltpu.VMEM((1, tok_count), jnp.float32),
                pltpu.VMEM((tok_count, dim), bf16),
                pltpu.VMEM((dim // LANE, tok_count, LANE), bf16),
                pltpu.VMEM((n_dev, cap, dim), bf16),
                pltpu.VMEM((n_dev, cap, dim), bf16),
                pltpu.VMEM((2, n_z * part, ffn), bf16),
                pltpu.VMEM((n_z * LANE, ffn), bf16),
                pltpu.VMEM((n_z * HALF, ffn), bf16),
                pltpu.VMEM((slots, ffn), bf16),
                pltpu.VMEM((n_dev, cap, n_z * LANE), bf16),
                pltpu.VMEM((n_dev, cap, n_z * HALF), bf16),
                pltpu.VMEM((n_dev, cap, n_z * LANE), bf16),
                pltpu.VMEM((n_dev, cap, n_z * HALF), bf16),
                pltpu.VMEM((tok_count, slots), bf16),
                dma((3,)), dma((4,)),
                dma((2, n_z - 1)), dma((CHUNKS, 2, n_z)), dma((n_z,)), dma((CHUNKS, n_z)),
                dma((2, DOWN_SPLIT, n_z - 1)), dma((2, DOWN_SPLIT, n_z)), dma((2, DOWN_SPLIT, n_z)), dma((2, DOWN_SPLIT, n_z)),
                dma((n_dev,)), dma((n_dev,)), dma((2, n_dev)), dma((2, n_dev)), dma((dim // LANE,)),
            ],
            compiler_params=pltpu.CompilerParams(
                collective_id=0, has_side_effects=True, vmem_limit_bytes=60 * 1024 * 1024),
            cost_estimate=pl.CostEstimate(
                flops=6 * slots * dim * ffn, bytes_accessed=6 * dim * ffn, transcendentals=slots * ffn),
        )(expert_idx.reshape(1, tok_count), gates.reshape(1, tok_count), tokens, w_gate, w_up, jnp.swapaxes(w_down, 1, 2))

    return jax.shard_map(
        device_step, mesh=mesh,
        in_specs=(row_spec, row_spec, row_spec, P("ep", "fsdp", None), P("ep", "fsdp", None), P("ep", None, "fsdp")),
        out_specs=row_spec, check_vma=False)
```

```python
import functools

import jax
import jax.numpy as jnp
from jax import lax
from jax.experimental import pallas as pl
from jax.experimental.pallas import tpu as pltpu
from jax.sharding import PartitionSpec as P

MESH = pl.DeviceIdType.MESH
LANE = 128
HALF = 64
CHUNKS = 6
AHEAD = 4
ROWS_AFTER = 3
STEPS = "RRRR H HR HR HR HR HR R F R f RR Ff"
DOWN_SPLIT = 3
ROW_BLOCKS = 4


def aligned(start, size, step):
    return pl.ds(pl.multiple_of(start * step, step), size)


def moe_kernel(n_rep, n_ep, n_z, cap, idx_ref, gate_ref, tok_ref, wg_ref, wu_ref, wd_ref, out_ref,
               idx_v, gate_v, tok_v, send_v, x_v, w_v, wd0_v, wd1_v, h_v, o0_v, o1_v, back0_v, back1_v, sel_v,
               tok_sem, own_sem, gsend, grecv, gpass_send, gpass_recv, dsend, drecv, dpass_send, dpass_recv,
               xsend, xrecv, bsend, brecv):
    rep, ep, z = lax.axis_index("rep"), lax.axis_index("ep"), lax.axis_index("fsdp")
    rep = rep if n_rep > 1 else 0
    me = ep * n_z + z
    n_dev = n_ep * n_z
    part, ffn = wg_ref.shape[1], wg_ref.shape[2]
    share, span = part // n_rep, ffn // n_rep // DOWN_SPLIT
    width = ffn // CHUNKS
    tok_count, dim = tok_ref.shape
    slots = n_dev * cap
    block, per_block = slots // ROW_BLOCKS, n_dev // ROW_BLOCKS
    gate_up = (wg_ref, wu_ref)
    wd_v, o_v, back_v = (wd0_v, wd1_v), (o0_v, o1_v), (back0_v, back1_v)
    group_rows = ((0, LANE), (LANE, HALF))
    other_rep = {"rep": lax.rem(rep + 1, n_rep)}

    def place(s):
        return {"ep": lax.div(s, n_z), "fsdp": lax.rem(s, n_z)}

    def remote(src, dst, send_sem, recv_sem, where):
        return pltpu.make_async_remote_copy(
            src_ref=src, dst_ref=dst, send_sem=send_sem, recv_sem=recv_sem, device_id=where, device_id_type=MESH)

    small = [pltpu.make_async_copy(ref, to, tok_sem.at[n])
             for n, (ref, to) in enumerate(((idx_ref, idx_v), (gate_ref, gate_v), (tok_ref, tok_v)))]
    own = []
    for k in range(2):
        own.append(pltpu.make_async_copy(gate_up[k].at[z], w_v.at[k, aligned(z, part, part), :], own_sem.at[k]))
    for g, (first, rows) in enumerate(group_rows):
        own.append(pltpu.make_async_copy(
            wd_ref.at[z, first:first + rows, :], wd_v[g].at[aligned(z, rows, rows), :], own_sem.at[2 + g]))
    for copy in small + own:
        copy.start()

    barrier = pltpu.get_barrier_semaphore()
    for d in range(1, n_dev):
        pl.semaphore_signal(barrier, inc=1, device_id=place(lax.rem(me + d, n_dev)), device_id_type=MESH)
    if n_rep > 1:
        pl.semaphore_signal(barrier, inc=1, device_id=other_rep, device_id_type=MESH)
    pl.semaphore_wait(barrier, n_dev - 1 + n_rep - 1)

    flip = lax.div(z, n_z // 2)

    def mirror(t):
        return t + flip * (n_z - 1 - 2 * t)

    peers = [mirror(t) for t in [1 - mirror(z)] + list(range(n_z // 2, n_z))]

    def share_rows(src, of_rep):
        return pl.ds(pl.multiple_of(src * part + of_rep * share, share), share)

    def gate_up_copy(k, p, cols, sem):
        zp = peers[p]
        return remote(gate_up[k].at[zp, aligned(rep, share, share), cols], w_v.at[k, share_rows(z, rep), cols],
                      gsend.at[k, p], sem, {"fsdp": zp})

    def gate_up_pass(src, of_rep, cols, sem):
        at = w_v.at[:, share_rows(src, of_rep), cols]
        return remote(at, at, gpass_send.at[src], sem, other_rep)

    def down_cols(of_rep, q):
        return aligned(of_rep * DOWN_SPLIT + q, span, span)

    def down_copy(g, q, p):
        zp = peers[p]
        first, rows = group_rows[g]
        cols = down_cols(rep, q)
        return remote(wd_ref.at[zp, first:first + rows, cols], wd_v[g].at[aligned(z, rows, rows), cols],
                      dsend.at[g, q, p], drecv.at[g, q, z], {"fsdp": zp})

    def down_pass(g, q, src, of_rep):
        rows = group_rows[g][1]
        at = wd_v[g].at[aligned(src, rows, rows), down_cols(of_rep, q)]
        return remote(at, at, dpass_send.at[g, q, src], dpass_recv.at[g, q, src], other_rep)

    def row_copy(s, at):
        return remote(send_v.at[s], x_v.at[at], xsend.at[s], xrecv.at[at], place(s))

    def back_copy(g, s, at):
        return remote(o_v[g].at[s], back_v[g].at[at], bsend.at[g, s], brecv.at[g, at], place(s))

    def for_others(run):
        def step(d, carry):
            first = lax.rem(ep + d, n_ep) * n_z

            @pl.when(d > 0)
            def _():
                run(first + z)

            for p in peers:
                run(first + p)
            return carry
        lax.fori_loop(0, n_ep, step, 0)

    def send(item):
        if item < CHUNKS:
            cols = pl.ds(item * width, width)
            for p in range(n_z - 1):
                for k in range(2):
                    gate_up_copy(k, p, cols, grecv.at[item, k, z]).start()
        elif item == CHUNKS:
            for_others(lambda s: row_copy(s, me).start())
        elif item <= CHUNKS + 2 * DOWN_SPLIT:
            g, q = divmod(item - CHUNKS - 1, DOWN_SPLIT)
            for p in range(n_z - 1):
                down_copy(g, q, p).start()

    def receive(item):
        if item < CHUNKS:
            cols = pl.ds(item * width, width)
            for src in peers:
                for k in range(2):
                    at = w_v.at[k, share_rows(src, rep), cols]
                    remote(at, at, gsend.at[k, 0], grecv.at[item, k, src], {"fsdp": src}).wait_recv()
                if n_rep > 1:
                    gate_up_pass(src, rep, cols, gpass_recv.at[item, src]).start()
        elif item == CHUNKS:
            for_others(lambda s: row_copy(s, s).wait())
        else:
            g, q = divmod(item - CHUNKS - 1, DOWN_SPLIT)
            for src in peers:
                rows = group_rows[g][1]
                at = wd_v[g].at[aligned(src, rows, rows), down_cols(rep, q)]
                remote(at, at, dsend.at[g, q, 0], drecv.at[g, q, src], {"fsdp": src}).wait_recv()
                if n_rep > 1:
                    down_pass(g, q, src, rep).start()

    def make_rows():
        small[0].wait()
        small[1].wait()
        ids = idx_v[...]
        onehot = (lax.broadcasted_iota(jnp.int32, (n_dev, tok_count), 0) == ids).astype(jnp.float32)
        earlier = (lax.broadcasted_iota(jnp.int32, (tok_count, tok_count), 0)
                   < lax.broadcasted_iota(jnp.int32, (tok_count, tok_count), 1)).astype(jnp.bfloat16)
        before = jnp.dot(onehot.astype(jnp.bfloat16), earlier, preferred_element_type=jnp.float32)
        slot = jnp.sum(before * onehot, axis=0, keepdims=True)
        target = jnp.where(slot < cap, ids.astype(jnp.float32) * cap + slot, -1.0)

        small[2].wait()

        def dispatch(i, carry):
            want = lax.broadcasted_iota(jnp.int32, (block, tok_count), 0) + i * block
            pick = (want.astype(jnp.float32) == target).astype(jnp.bfloat16)
            picked = jnp.dot(pick, tok_v[...], preferred_element_type=jnp.float32).astype(jnp.bfloat16)
            send_v[pl.ds(i * per_block, per_block)] = picked.reshape(per_block, cap, dim)
            return carry

        lax.fori_loop(0, ROW_BLOCKS, dispatch, 0)
        x_v[me] = send_v[me]

        spread = jnp.transpose(jnp.broadcast_to(target, (LANE, tok_count)))
        for j in range(slots // LANE):
            want = lax.broadcasted_iota(jnp.int32, (tok_count, LANE), 1) + j * LANE
            sel_v[:, j * LANE:(j + 1) * LANE] = (spread == want.astype(jnp.float32)).astype(jnp.bfloat16)

    order = list(range(CHUNKS))
    order = order[:ROWS_AFTER] + [CHUNKS] + order[ROWS_AFTER:] + [CHUNKS + 1 + i for i in range(2 * DOWN_SPLIT)]
    for item in order[:AHEAD]:
        if item == CHUNKS:
            make_rows()
        send(item)
    if CHUNKS not in order[:AHEAD]:
        make_rows()

    at_item = iter(range(len(order)))

    def receive_next():
        n = next(at_item)
        receive(order[n])
        if n + AHEAD < len(order):
            send(order[n + AHEAD])

    def hidden_chunk(c):
        cols = slice(c * width, (c + 1) * width)
        if c == 0:
            for copy in own:
                copy.wait()
        if n_rep > 1:
            for src in peers:
                gate_up_pass(src, 1 - rep, pl.ds(c * width, width), gpass_recv.at[c, src]).wait_recv()

        def hidden(i, carry, cols=cols):
            x = x_v[pl.ds(i * per_block, per_block)].reshape(block, dim)
            a = jnp.dot(x, w_v[0, :, cols], preferred_element_type=jnp.float32)
            b = jnp.dot(x, w_v[1, :, cols], preferred_element_type=jnp.float32)
            h_v[aligned(i, block, block), cols] = (a * jax.nn.sigmoid(a) * b).astype(jnp.bfloat16)
            return carry

        lax.fori_loop(0, ROW_BLOCKS, hidden, 0)

    def finish(g, half):
        if n_rep > 1 and half == 0:
            for q in range(DOWN_SPLIT):
                for src in peers:
                    down_pass(g, q, src, 1 - rep).wait_recv()

        def send_back(i):
            for p in peers:
                back_copy(g, i * per_block + p, me).start()

            @pl.when(i != ep)
            def _():
                back_copy(g, i * per_block + z, me).start()

        def rows_out(n, carry):
            i = lax.rem(ep + n, ROW_BLOCKS)
            total = lax.dot_general(h_v[aligned(i, block, block), :], wd_v[g][...], (((1,), (1,)), ((), ())),
                                    preferred_element_type=jnp.float32)
            o_v[g][pl.ds(i * per_block, per_block)] = total.astype(jnp.bfloat16).reshape(
                per_block, cap, n_z * group_rows[g][1])

            @pl.when(n > 0)
            def _():
                send_back(lax.rem(i + ROW_BLOCKS - 1, ROW_BLOCKS))

            return carry

        lax.fori_loop(half * ROW_BLOCKS // 2, (half + 1) * ROW_BLOCKS // 2, rows_out, 0)
        if half == 1:
            back_v[g][me] = o_v[g][me]
            send_back(lax.rem(ep + ROW_BLOCKS - 1, ROW_BLOCKS))

    chunk_count, group_count = iter(range(CHUNKS)), iter((0, 0, 1, 1))
    for step in STEPS.replace(" ", ""):
        if step == "R":
            receive_next()
        elif step == "H":
            hidden_chunk(next(chunk_count))
        else:
            finish(next(group_count), int(step == "f"))

    every = pl.ds(0, ffn)
    for p in range(n_z - 1):
        for k in range(2):
            gate_up_copy(k, p, every, grecv.at[0, k, z]).wait_send()
        for g in range(2):
            for q in range(DOWN_SPLIT):
                down_copy(g, q, p).wait_send()
        if n_rep > 1:
            gate_up_pass(peers[p], rep, every, gpass_recv.at[0, peers[p]]).wait_send()
            for g in range(2):
                for q in range(DOWN_SPLIT):
                    down_pass(g, q, peers[p], rep).wait_send()

    scale = jnp.transpose(jnp.broadcast_to(gate_v[...], (LANE, tok_count)))
    low_lanes = lax.broadcasted_iota(jnp.int32, (tok_count, LANE), 1) < HALF
    mixed = []

    def piece(half):
        src, j = divmod(half, part // HALF)
        g, start = (0, src * LANE) if j < 2 else (1, (src // 2) * LANE)
        return mixed[g][:, start:start + LANE], j if j < 2 else src % 2

    def put(t):
        (low, low_at), (high, high_at) = piece(2 * t), piece(2 * t + 1)
        low = low if low_at == 0 else pltpu.roll(low, HALF, 1)
        high = high if high_at == 1 else pltpu.roll(high, HALF, 1)
        cols = slice(t * LANE, (t + 1) * LANE)
        value = jnp.where(low_lanes, low, high)
        out_ref[:, cols] = (tok_v[:, cols].astype(jnp.float32) + scale * value).astype(jnp.bfloat16)

    only_first = [t for t in range(dim // LANE) if (2 * t) % 3 < 2 and (2 * t + 1) % 3 < 2]
    for g in range(2):
        for_others(lambda s, g=g: back_copy(g, s, s).wait())
        mixed.append(jnp.dot(sel_v[...], back_v[g][...].reshape(slots, n_z * group_rows[g][1]),
                             preferred_element_type=jnp.float32))
        for t in range(dim // LANE):
            if (t in only_first) == (g == 0):
                put(t)


def solution(mesh):
    n_rep, n_ep, n_z = mesh.shape["rep"], mesh.shape["ep"], mesh.shape["fsdp"]
    row_spec = P(("rep", "ep", "fsdp"), None)

    def device_step(tokens, expert_idx, gates, w_gate, w_up, w_down):
        tok_count, top_k = expert_idx.shape
        n_local, part, ffn = w_gate.shape
        dim = tokens.shape[1]
        assert top_k == 1 and n_local == n_z and n_ep == ROW_BLOCKS and n_z == 4 and part == LANE + HALF and n_rep <= 2
        n_dev = n_ep * n_z
        cap = (2 * tok_count + n_dev - 1) // n_dev
        slots = n_dev * cap
        any_spec = pl.BlockSpec(memory_space=pl.ANY)
        dma, bf16 = pltpu.SemaphoreType.DMA, jnp.bfloat16
        return pl.pallas_call(
            functools.partial(moe_kernel, n_rep, n_ep, n_z, cap),
            out_shape=pltpu.VMEM((tok_count, dim), bf16),
            in_specs=[any_spec, any_spec, any_spec, any_spec, any_spec, any_spec],
            out_specs=pl.BlockSpec(memory_space=pltpu.VMEM),
            scratch_shapes=[
                pltpu.VMEM((1, tok_count), jnp.int32),
                pltpu.VMEM((1, tok_count), jnp.float32),
                pltpu.VMEM((tok_count, dim), bf16),
                pltpu.VMEM((n_dev, cap, dim), bf16),
                pltpu.VMEM((n_dev, cap, dim), bf16),
                pltpu.VMEM((2, n_z * part, ffn), bf16),
                pltpu.VMEM((n_z * LANE, ffn), bf16),
                pltpu.VMEM((n_z * HALF, ffn), bf16),
                pltpu.VMEM((slots, ffn), bf16),
                pltpu.VMEM((n_dev, cap, n_z * LANE), bf16),
                pltpu.VMEM((n_dev, cap, n_z * HALF), bf16),
                pltpu.VMEM((n_dev, cap, n_z * LANE), bf16),
                pltpu.VMEM((n_dev, cap, n_z * HALF), bf16),
                pltpu.VMEM((tok_count, slots), bf16),
                dma((3,)), dma((4,)),
                dma((2, n_z - 1)), dma((CHUNKS, 2, n_z)), dma((n_z,)), dma((CHUNKS, n_z)),
                dma((2, DOWN_SPLIT, n_z - 1)), dma((2, DOWN_SPLIT, n_z)), dma((2, DOWN_SPLIT, n_z)), dma((2, DOWN_SPLIT, n_z)),
                dma((n_dev,)), dma((n_dev,)), dma((2, n_dev)), dma((2, n_dev)),
            ],
            compiler_params=pltpu.CompilerParams(
                collective_id=0, has_side_effects=True, vmem_limit_bytes=60 * 1024 * 1024),
            cost_estimate=pl.CostEstimate(
                flops=6 * slots * dim * ffn, bytes_accessed=6 * dim * ffn, transcendentals=slots * ffn),
        )(expert_idx.reshape(1, tok_count), gates.reshape(1, tok_count), tokens, w_gate, w_up, jnp.swapaxes(w_down, 1, 2))

    return jax.shard_map(
        device_step, mesh=mesh,
        in_specs=(row_spec, row_spec, row_spec, P("ep", "fsdp", None), P("ep", "fsdp", None), P("ep", None, "fsdp")),
        out_specs=row_spec, check_vma=False)
```

```python
import functools

import jax
import jax.numpy as jnp
from jax import lax
from jax.experimental import pallas as pl
from jax.experimental.pallas import tpu as pltpu
from jax.sharding import PartitionSpec as P

MESH = pl.DeviceIdType.MESH
LANE = 128
HALF = 64
CHUNKS = 6
AHEAD = 5
ROWS_AFTER = 2
STEPS = "RRRHRHRHRHRHRHRRFRfRRFf"
DOWN_SPLIT = 3
ROW_BLOCKS = 4


def aligned(start, size, step):
    return pl.ds(pl.multiple_of(start * step, step), size)


def moe_kernel(n_rep, n_ep, n_z, cap, idx_ref, gate_ref, tok_ref, wg_ref, wu_ref, wd_ref, out_ref,
               idx_v, gate_v, tok_v, send_v, x_v, w_v, wd0_v, wd1_v, h_v, o0_v, o1_v, back0_v, back1_v, sel_v,
               tok_sem, own_sem, gsend, grecv, gpass_send, gpass_recv, dsend, drecv, dpass_send, dpass_recv,
               xsend, xrecv, bsend, brecv):
    rep, ep, z = lax.axis_index("rep"), lax.axis_index("ep"), lax.axis_index("fsdp")
    rep = rep if n_rep > 1 else 0
    me = ep * n_z + z
    n_dev = n_ep * n_z
    part, ffn = wg_ref.shape[1], wg_ref.shape[2]
    share, span = part // n_rep, ffn // n_rep // DOWN_SPLIT
    width = ffn // CHUNKS
    tok_count, dim = tok_ref.shape
    slots = n_dev * cap
    block, per_block = slots // ROW_BLOCKS, n_dev // ROW_BLOCKS
    gate_up = (wg_ref, wu_ref)
    wd_v, o_v, back_v = (wd0_v, wd1_v), (o0_v, o1_v), (back0_v, back1_v)
    group_rows = ((0, LANE), (LANE, HALF))
    other_rep = {"rep": lax.rem(rep + 1, n_rep)}

    def place(s):
        return {"ep": lax.div(s, n_z), "fsdp": lax.rem(s, n_z)}

    def remote(src, dst, send_sem, recv_sem, where):
        return pltpu.make_async_remote_copy(
            src_ref=src, dst_ref=dst, send_sem=send_sem, recv_sem=recv_sem, device_id=where, device_id_type=MESH)

    small = [pltpu.make_async_copy(ref, to, tok_sem.at[n])
             for n, (ref, to) in enumerate(((idx_ref, idx_v), (gate_ref, gate_v), (tok_ref, tok_v)))]
    own = []
    for k in range(2):
        own.append(pltpu.make_async_copy(gate_up[k].at[z], w_v.at[k, aligned(z, part, part), :], own_sem.at[k]))
    for g, (first, rows) in enumerate(group_rows):
        own.append(pltpu.make_async_copy(
            wd_ref.at[z, first:first + rows, :], wd_v[g].at[aligned(z, rows, rows), :], own_sem.at[2 + g]))
    for copy in small + own:
        copy.start()

    barrier = pltpu.get_barrier_semaphore()
    for d in range(1, n_dev):
        pl.semaphore_signal(barrier, inc=1, device_id=place(lax.rem(me + d, n_dev)), device_id_type=MESH)
    if n_rep > 1:
        pl.semaphore_signal(barrier, inc=1, device_id=other_rep, device_id_type=MESH)
    pl.semaphore_wait(barrier, n_dev - 1 + n_rep - 1)

    flip = lax.div(z, n_z // 2)

    def mirror(t):
        return t + flip * (n_z - 1 - 2 * t)

    peers = [mirror(t) for t in [1 - mirror(z)] + list(range(n_z // 2, n_z))]

    def share_rows(src, of_rep):
        return pl.ds(pl.multiple_of(src * part + of_rep * share, share), share)

    def gate_up_copy(k, p, cols, sem):
        zp = peers[p]
        return remote(gate_up[k].at[zp, aligned(rep, share, share), cols], w_v.at[k, share_rows(z, rep), cols],
                      gsend.at[k, p], sem, {"fsdp": zp})

    def gate_up_pass(src, of_rep, cols, sem):
        at = w_v.at[:, share_rows(src, of_rep), cols]
        return remote(at, at, gpass_send.at[src], sem, other_rep)

    def down_cols(of_rep, q):
        return aligned(of_rep * DOWN_SPLIT + q, span, span)

    def down_copy(g, q, p):
        zp = peers[p]
        first, rows = group_rows[g]
        cols = down_cols(rep, q)
        return remote(wd_ref.at[zp, first:first + rows, cols], wd_v[g].at[aligned(z, rows, rows), cols],
                      dsend.at[g, q, p], drecv.at[g, q, z], {"fsdp": zp})

    def down_pass(g, q, src, of_rep):
        rows = group_rows[g][1]
        at = wd_v[g].at[aligned(src, rows, rows), down_cols(of_rep, q)]
        return remote(at, at, dpass_send.at[g, q, src], dpass_recv.at[g, q, src], other_rep)

    def row_copy(s, at):
        return remote(send_v.at[s], x_v.at[at], xsend.at[s], xrecv.at[at], place(s))

    def back_copy(g, s, at):
        return remote(o_v[g].at[s], back_v[g].at[at], bsend.at[g, s], brecv.at[g, at], place(s))

    def for_others(run):
        def step(d, carry):
            first = lax.rem(ep + d, n_ep) * n_z

            @pl.when(d > 0)
            def _():
                run(first + z)

            for p in peers:
                run(first + p)
            return carry
        lax.fori_loop(0, n_ep, step, 0)

    def send(item):
        if item < CHUNKS:
            cols = pl.ds(item * width, width)
            for p in range(n_z - 1):
                for k in range(2):
                    gate_up_copy(k, p, cols, grecv.at[item, k, z]).start()
        elif item == CHUNKS:
            for_others(lambda s: row_copy(s, me).start())
        elif item <= CHUNKS + 2 * DOWN_SPLIT:
            g, q = divmod(item - CHUNKS - 1, DOWN_SPLIT)
            for p in range(n_z - 1):
                down_copy(g, q, p).start()

    def receive(item):
        if item < CHUNKS:
            cols = pl.ds(item * width, width)
            for src in peers:
                for k in range(2):
                    at = w_v.at[k, share_rows(src, rep), cols]
                    remote(at, at, gsend.at[k, 0], grecv.at[item, k, src], {"fsdp": src}).wait_recv()
                if n_rep > 1:
                    gate_up_pass(src, rep, cols, gpass_recv.at[item, src]).start()
        elif item == CHUNKS:
            for_others(lambda s: row_copy(s, s).wait())
        else:
            g, q = divmod(item - CHUNKS - 1, DOWN_SPLIT)
            for src in peers:
                rows = group_rows[g][1]
                at = wd_v[g].at[aligned(src, rows, rows), down_cols(rep, q)]
                remote(at, at, dsend.at[g, q, 0], drecv.at[g, q, src], {"fsdp": src}).wait_recv()
                if n_rep > 1:
                    down_pass(g, q, src, rep).start()

    def make_rows():
        small[0].wait()
        small[1].wait()
        ids = idx_v[...]
        onehot = (lax.broadcasted_iota(jnp.int32, (n_dev, tok_count), 0) == ids).astype(jnp.float32)
        earlier = (lax.broadcasted_iota(jnp.int32, (tok_count, tok_count), 0)
                   < lax.broadcasted_iota(jnp.int32, (tok_count, tok_count), 1)).astype(jnp.bfloat16)
        before = jnp.dot(onehot.astype(jnp.bfloat16), earlier, preferred_element_type=jnp.float32)
        slot = jnp.sum(before * onehot, axis=0, keepdims=True)
        target = jnp.where(slot < cap, ids.astype(jnp.float32) * cap + slot, -1.0)

        small[2].wait()

        def dispatch(i, carry):
            want = lax.broadcasted_iota(jnp.int32, (block, tok_count), 0) + i * block
            pick = (want.astype(jnp.float32) == target).astype(jnp.bfloat16)
            picked = jnp.dot(pick, tok_v[...], preferred_element_type=jnp.float32).astype(jnp.bfloat16)
            send_v[pl.ds(i * per_block, per_block)] = picked.reshape(per_block, cap, dim)
            return carry

        lax.fori_loop(0, ROW_BLOCKS, dispatch, 0)
        x_v[me] = send_v[me]

        spread = jnp.transpose(jnp.broadcast_to(target, (LANE, tok_count)))
        for j in range(slots // LANE):
            want = lax.broadcasted_iota(jnp.int32, (tok_count, LANE), 1) + j * LANE
            sel_v[:, j * LANE:(j + 1) * LANE] = (spread == want.astype(jnp.float32)).astype(jnp.bfloat16)

    order = list(range(CHUNKS))
    order = order[:ROWS_AFTER] + [CHUNKS] + order[ROWS_AFTER:] + [CHUNKS + 1 + i for i in range(2 * DOWN_SPLIT)]
    for item in order[:AHEAD]:
        if item == CHUNKS:
            make_rows()
        send(item)
    if CHUNKS not in order[:AHEAD]:
        make_rows()

    at_item = iter(range(len(order)))

    def receive_next():
        n = next(at_item)
        receive(order[n])
        if n + AHEAD < len(order):
            send(order[n + AHEAD])

    def hidden_chunk(c):
        cols = slice(c * width, (c + 1) * width)
        if c == 0:
            for copy in own:
                copy.wait()
        if n_rep > 1:
            for src in peers:
                gate_up_pass(src, 1 - rep, pl.ds(c * width, width), gpass_recv.at[c, src]).wait_recv()

        def hidden(i, carry, cols=cols):
            x = x_v[pl.ds(i * per_block, per_block)].reshape(block, dim)
            a = jnp.dot(x, w_v[0, :, cols], preferred_element_type=jnp.float32)
            b = jnp.dot(x, w_v[1, :, cols], preferred_element_type=jnp.float32)
            h_v[aligned(i, block, block), cols] = (a * jax.nn.sigmoid(a) * b).astype(jnp.bfloat16)
            return carry

        lax.fori_loop(0, ROW_BLOCKS, hidden, 0)

    def finish(g, half):
        if n_rep > 1 and half == 0:
            for q in range(DOWN_SPLIT):
                for src in peers:
                    down_pass(g, q, src, 1 - rep).wait_recv()

        def send_back(i):
            for p in peers:
                back_copy(g, i * per_block + p, me).start()

            @pl.when(i != ep)
            def _():
                back_copy(g, i * per_block + z, me).start()

        def rows_out(n, carry):
            i = lax.rem(ep + n, ROW_BLOCKS)
            total = lax.dot_general(h_v[aligned(i, block, block), :], wd_v[g][...], (((1,), (1,)), ((), ())),
                                    preferred_element_type=jnp.float32)
            o_v[g][pl.ds(i * per_block, per_block)] = total.astype(jnp.bfloat16).reshape(
                per_block, cap, n_z * group_rows[g][1])

            @pl.when(n > 0)
            def _():
                send_back(lax.rem(i + ROW_BLOCKS - 1, ROW_BLOCKS))

            return carry

        lax.fori_loop(half * ROW_BLOCKS // 2, (half + 1) * ROW_BLOCKS // 2, rows_out, 0)
        if half == 1:
            back_v[g][me] = o_v[g][me]
            send_back(lax.rem(ep + ROW_BLOCKS - 1, ROW_BLOCKS))

    chunk_count, group_count = iter(range(CHUNKS)), iter((0, 0, 1, 1))
    for step in STEPS:
        if step == "R":
            receive_next()
        elif step == "H":
            hidden_chunk(next(chunk_count))
        else:
            finish(next(group_count), int(step == "f"))

    every = pl.ds(0, ffn)
    for p in range(n_z - 1):
        for k in range(2):
            gate_up_copy(k, p, every, grecv.at[0, k, z]).wait_send()
        for g in range(2):
            for q in range(DOWN_SPLIT):
                down_copy(g, q, p).wait_send()
        if n_rep > 1:
            gate_up_pass(peers[p], rep, every, gpass_recv.at[0, peers[p]]).wait_send()
            for g in range(2):
                for q in range(DOWN_SPLIT):
                    down_pass(g, q, peers[p], rep).wait_send()

    scale = jnp.transpose(jnp.broadcast_to(gate_v[...], (LANE, tok_count)))
    low_lanes = lax.broadcasted_iota(jnp.int32, (tok_count, LANE), 1) < HALF
    mixed = []

    def piece(half):
        src, j = divmod(half, part // HALF)
        g, start = (0, src * LANE) if j < 2 else (1, (src // 2) * LANE)
        return mixed[g][:, start:start + LANE], j if j < 2 else src % 2

    def put(t):
        (low, low_at), (high, high_at) = piece(2 * t), piece(2 * t + 1)
        low = low if low_at == 0 else pltpu.roll(low, HALF, 1)
        high = high if high_at == 1 else pltpu.roll(high, HALF, 1)
        cols = slice(t * LANE, (t + 1) * LANE)
        value = jnp.where(low_lanes, low, high)
        out_ref[:, cols] = (tok_v[:, cols].astype(jnp.float32) + scale * value).astype(jnp.bfloat16)

    only_first = [t for t in range(dim // LANE) if (2 * t) % 3 < 2 and (2 * t + 1) % 3 < 2]
    for g in range(2):
        for_others(lambda s, g=g: back_copy(g, s, s).wait())
        mixed.append(jnp.dot(sel_v[...], back_v[g][...].reshape(slots, n_z * group_rows[g][1]),
                             preferred_element_type=jnp.float32))
        for t in range(dim // LANE):
            if (t in only_first) == (g == 0):
                put(t)


def solution(mesh):
    n_rep, n_ep, n_z = mesh.shape["rep"], mesh.shape["ep"], mesh.shape["fsdp"]
    row_spec = P(("rep", "ep", "fsdp"), None)

    def device_step(tokens, expert_idx, gates, w_gate, w_up, w_down):
        tok_count, top_k = expert_idx.shape
        n_local, part, ffn = w_gate.shape
        dim = tokens.shape[1]
        assert top_k == 1 and n_local == n_z and n_ep == ROW_BLOCKS and n_z == 4 and part == LANE + HALF and n_rep <= 2
        n_dev = n_ep * n_z
        cap = (2 * tok_count + n_dev - 1) // n_dev
        slots = n_dev * cap
        any_spec = pl.BlockSpec(memory_space=pl.ANY)
        dma, bf16 = pltpu.SemaphoreType.DMA, jnp.bfloat16
        return pl.pallas_call(
            functools.partial(moe_kernel, n_rep, n_ep, n_z, cap),
            out_shape=pltpu.VMEM((tok_count, dim), bf16),
            in_specs=[any_spec, any_spec, any_spec, any_spec, any_spec, any_spec],
            out_specs=pl.BlockSpec(memory_space=pltpu.VMEM),
            scratch_shapes=[
                pltpu.VMEM((1, tok_count), jnp.int32),
                pltpu.VMEM((1, tok_count), jnp.float32),
                pltpu.VMEM((tok_count, dim), bf16),
                pltpu.VMEM((n_dev, cap, dim), bf16),
                pltpu.VMEM((n_dev, cap, dim), bf16),
                pltpu.VMEM((2, n_z * part, ffn), bf16),
                pltpu.VMEM((n_z * LANE, ffn), bf16),
                pltpu.VMEM((n_z * HALF, ffn), bf16),
                pltpu.VMEM((slots, ffn), bf16),
                pltpu.VMEM((n_dev, cap, n_z * LANE), bf16),
                pltpu.VMEM((n_dev, cap, n_z * HALF), bf16),
                pltpu.VMEM((n_dev, cap, n_z * LANE), bf16),
                pltpu.VMEM((n_dev, cap, n_z * HALF), bf16),
                pltpu.VMEM((tok_count, slots), bf16),
                dma((3,)), dma((4,)),
                dma((2, n_z - 1)), dma((CHUNKS, 2, n_z)), dma((n_z,)), dma((CHUNKS, n_z)),
                dma((2, DOWN_SPLIT, n_z - 1)), dma((2, DOWN_SPLIT, n_z)), dma((2, DOWN_SPLIT, n_z)), dma((2, DOWN_SPLIT, n_z)),
                dma((n_dev,)), dma((n_dev,)), dma((2, n_dev)), dma((2, n_dev)),
            ],
            compiler_params=pltpu.CompilerParams(
                collective_id=0, has_side_effects=True, vmem_limit_bytes=60 * 1024 * 1024),
            cost_estimate=pl.CostEstimate(
                flops=6 * slots * dim * ffn, bytes_accessed=6 * dim * ffn, transcendentals=slots * ffn),
        )(expert_idx.reshape(1, tok_count), gates.reshape(1, tok_count), tokens, w_gate, w_up, jnp.swapaxes(w_down, 1, 2))

    return jax.shard_map(
        device_step, mesh=mesh,
        in_specs=(row_spec, row_spec, row_spec, P("ep", "fsdp", None), P("ep", "fsdp", None), P("ep", None, "fsdp")),
        out_specs=row_spec, check_vma=False)
```

```python
import functools

import jax
import jax.numpy as jnp
from jax import lax
from jax.experimental import pallas as pl
from jax.experimental.pallas import tpu as pltpu
from jax.sharding import PartitionSpec as P

MESH = pl.DeviceIdType.MESH
LANE = 128
HALF = 64
CHUNKS = 6
AHEAD = 4
ROWS_AFTER = 3
STEPS = "RRRRHHRHRHRHRHRRFRfRRFf"
DOWN_SPLIT = 3
ROW_BLOCKS = 4


def aligned(start, size, step):
    return pl.ds(pl.multiple_of(start * step, step), size)


def moe_kernel(n_rep, n_ep, n_z, cap, idx_ref, gate_ref, tok_ref, wg_ref, wu_ref, wd_ref, out_ref,
               idx_v, gate_v, tok_v, send_v, x_v, w_v, wd0_v, wd1_v, h_v, o0_v, o1_v, back0_v, back1_v, sel_v,
               tok_sem, own_sem, gsend, grecv, gpass_send, gpass_recv, dsend, drecv, dpass_send, dpass_recv,
               xsend, xrecv, bsend, brecv):
    rep, ep, z = lax.axis_index("rep"), lax.axis_index("ep"), lax.axis_index("fsdp")
    rep = rep if n_rep > 1 else 0
    me = ep * n_z + z
    n_dev = n_ep * n_z
    part, ffn = wg_ref.shape[1], wg_ref.shape[2]
    share, span = part // n_rep, ffn // n_rep // DOWN_SPLIT
    width = ffn // CHUNKS
    tok_count, dim = tok_ref.shape
    slots = n_dev * cap
    block, per_block = slots // ROW_BLOCKS, n_dev // ROW_BLOCKS
    gate_up = (wg_ref, wu_ref)
    wd_v, o_v, back_v = (wd0_v, wd1_v), (o0_v, o1_v), (back0_v, back1_v)
    group_rows = ((0, LANE), (LANE, HALF))
    other_rep = {"rep": lax.rem(rep + 1, n_rep)}

    def place(s):
        return {"ep": lax.div(s, n_z), "fsdp": lax.rem(s, n_z)}

    def remote(src, dst, send_sem, recv_sem, where):
        return pltpu.make_async_remote_copy(
            src_ref=src, dst_ref=dst, send_sem=send_sem, recv_sem=recv_sem, device_id=where, device_id_type=MESH)

    small = [pltpu.make_async_copy(ref, to, tok_sem.at[n])
             for n, (ref, to) in enumerate(((idx_ref, idx_v), (gate_ref, gate_v), (tok_ref, tok_v)))]
    own = []
    for k in range(2):
        own.append(pltpu.make_async_copy(gate_up[k].at[z], w_v.at[k, aligned(z, part, part), :], own_sem.at[k]))
    for g, (first, rows) in enumerate(group_rows):
        own.append(pltpu.make_async_copy(
            wd_ref.at[z, first:first + rows, :], wd_v[g].at[aligned(z, rows, rows), :], own_sem.at[2 + g]))
    for copy in small + own:
        copy.start()

    barrier = pltpu.get_barrier_semaphore()
    for d in range(1, n_dev):
        pl.semaphore_signal(barrier, inc=1, device_id=place(lax.rem(me + d, n_dev)), device_id_type=MESH)
    if n_rep > 1:
        pl.semaphore_signal(barrier, inc=1, device_id=other_rep, device_id_type=MESH)
    pl.semaphore_wait(barrier, n_dev - 1 + n_rep - 1)

    flip = lax.div(z, n_z // 2)

    def mirror(t):
        return t + flip * (n_z - 1 - 2 * t)

    peers = [mirror(t) for t in [1 - mirror(z)] + list(range(n_z // 2, n_z))]

    def share_rows(src, of_rep):
        return pl.ds(pl.multiple_of(src * part + of_rep * share, share), share)

    def gate_up_copy(k, p, cols, sem):
        zp = peers[p]
        return remote(gate_up[k].at[zp, aligned(rep, share, share), cols], w_v.at[k, share_rows(z, rep), cols],
                      gsend.at[k, p], sem, {"fsdp": zp})

    def gate_up_pass(src, of_rep, cols, sem):
        at = w_v.at[:, share_rows(src, of_rep), cols]
        return remote(at, at, gpass_send.at[src], sem, other_rep)

    def down_cols(of_rep, q):
        return aligned(of_rep * DOWN_SPLIT + q, span, span)

    def down_copy(g, q, p):
        zp = peers[p]
        first, rows = group_rows[g]
        cols = down_cols(rep, q)
        return remote(wd_ref.at[zp, first:first + rows, cols], wd_v[g].at[aligned(z, rows, rows), cols],
                      dsend.at[g, q, p], drecv.at[g, q, z], {"fsdp": zp})

    def down_pass(g, q, src, of_rep):
        rows = group_rows[g][1]
        at = wd_v[g].at[aligned(src, rows, rows), down_cols(of_rep, q)]
        return remote(at, at, dpass_send.at[g, q, src], dpass_recv.at[g, q, src], other_rep)

    def row_copy(s, at):
        return remote(send_v.at[s], x_v.at[at], xsend.at[s], xrecv.at[at], place(s))

    def back_copy(g, s, at):
        return remote(o_v[g].at[s], back_v[g].at[at], bsend.at[g, s], brecv.at[g, at], place(s))

    def for_others(run):
        def step(d, carry):
            first = lax.rem(ep + d, n_ep) * n_z

            @pl.when(d > 0)
            def _():
                run(first + z)

            for p in peers:
                run(first + p)
            return carry
        lax.fori_loop(0, n_ep, step, 0)

    def send(item):
        if item < CHUNKS:
            cols = pl.ds(item * width, width)
            for p in range(n_z - 1):
                for k in range(2):
                    gate_up_copy(k, p, cols, grecv.at[item, k, z]).start()
        elif item == CHUNKS:
            for_others(lambda s: row_copy(s, me).start())
        elif item <= CHUNKS + 2 * DOWN_SPLIT:
            g, q = divmod(item - CHUNKS - 1, DOWN_SPLIT)
            for p in range(n_z - 1):
                down_copy(g, q, p).start()

    def receive(item):
        if item < CHUNKS:
            cols = pl.ds(item * width, width)
            for src in peers:
                for k in range(2):
                    at = w_v.at[k, share_rows(src, rep), cols]
                    remote(at, at, gsend.at[k, 0], grecv.at[item, k, src], {"fsdp": src}).wait_recv()
                if n_rep > 1:
                    gate_up_pass(src, rep, cols, gpass_recv.at[item, src]).start()
        elif item == CHUNKS:
            for_others(lambda s: row_copy(s, s).wait())
        else:
            g, q = divmod(item - CHUNKS - 1, DOWN_SPLIT)
            for src in peers:
                rows = group_rows[g][1]
                at = wd_v[g].at[aligned(src, rows, rows), down_cols(rep, q)]
                remote(at, at, dsend.at[g, q, 0], drecv.at[g, q, src], {"fsdp": src}).wait_recv()
                if n_rep > 1:
                    down_pass(g, q, src, rep).start()

    def make_rows():
        small[0].wait()
        small[1].wait()
        ids = idx_v[...]
        onehot = (lax.broadcasted_iota(jnp.int32, (n_dev, tok_count), 0) == ids).astype(jnp.float32)
        earlier = (lax.broadcasted_iota(jnp.int32, (tok_count, tok_count), 0)
                   < lax.broadcasted_iota(jnp.int32, (tok_count, tok_count), 1)).astype(jnp.bfloat16)
        before = jnp.dot(onehot.astype(jnp.bfloat16), earlier, preferred_element_type=jnp.float32)
        slot = jnp.sum(before * onehot, axis=0, keepdims=True)
        target = jnp.where(slot < cap, ids.astype(jnp.float32) * cap + slot, -1.0)

        small[2].wait()

        def dispatch(i, carry):
            want = lax.broadcasted_iota(jnp.int32, (block, tok_count), 0) + i * block
            pick = (want.astype(jnp.float32) == target).astype(jnp.bfloat16)
            picked = jnp.dot(pick, tok_v[...], preferred_element_type=jnp.float32).astype(jnp.bfloat16)
            send_v[pl.ds(i * per_block, per_block)] = picked.reshape(per_block, cap, dim)
            return carry

        lax.fori_loop(0, ROW_BLOCKS, dispatch, 0)
        x_v[me] = send_v[me]

        spread = jnp.transpose(jnp.broadcast_to(target, (LANE, tok_count)))
        for j in range(slots // LANE):
            want = lax.broadcasted_iota(jnp.int32, (tok_count, LANE), 1) + j * LANE
            sel_v[:, j * LANE:(j + 1) * LANE] = (spread == want.astype(jnp.float32)).astype(jnp.bfloat16)

    order = list(range(CHUNKS))
    order = order[:ROWS_AFTER] + [CHUNKS] + order[ROWS_AFTER:] + [CHUNKS + 1 + i for i in range(2 * DOWN_SPLIT)]
    for item in order[:AHEAD]:
        if item == CHUNKS:
            make_rows()
        send(item)
    if CHUNKS not in order[:AHEAD]:
        make_rows()

    at_item = iter(range(len(order)))

    def receive_next():
        n = next(at_item)
        receive(order[n])
        if n + AHEAD < len(order):
            send(order[n + AHEAD])

    def hidden_chunk(c):
        cols = slice(c * width, (c + 1) * width)
        if c == 0:
            for copy in own:
                copy.wait()
        if n_rep > 1:
            for src in peers:
                gate_up_pass(src, 1 - rep, pl.ds(c * width, width), gpass_recv.at[c, src]).wait_recv()

        def hidden(i, carry, cols=cols):
            x = x_v[pl.ds(i * per_block, per_block)].reshape(block, dim)
            a = jnp.dot(x, w_v[0, :, cols], preferred_element_type=jnp.float32)
            b = jnp.dot(x, w_v[1, :, cols], preferred_element_type=jnp.float32)
            h_v[aligned(i, block, block), cols] = (a * jax.nn.sigmoid(a) * b).astype(jnp.bfloat16)
            return carry

        lax.fori_loop(0, ROW_BLOCKS, hidden, 0)

    def finish(g, half):
        if n_rep > 1 and half == 0:
            for q in range(DOWN_SPLIT):
                for src in peers:
                    down_pass(g, q, src, 1 - rep).wait_recv()

        def send_back(i):
            for p in peers:
                back_copy(g, i * per_block + p, me).start()

            @pl.when(i != ep)
            def _():
                back_copy(g, i * per_block + z, me).start()

        def rows_out(n, carry):
            i = lax.rem(ep + n, ROW_BLOCKS)
            total = lax.dot_general(h_v[aligned(i, block, block), :], wd_v[g][...], (((1,), (1,)), ((), ())),
                                    preferred_element_type=jnp.float32)
            o_v[g][pl.ds(i * per_block, per_block)] = total.astype(jnp.bfloat16).reshape(
                per_block, cap, n_z * group_rows[g][1])

            @pl.when(n > 0)
            def _():
                send_back(lax.rem(i + ROW_BLOCKS - 1, ROW_BLOCKS))

            return carry

        lax.fori_loop(half * ROW_BLOCKS // 2, (half + 1) * ROW_BLOCKS // 2, rows_out, 0)
        if half == 1:
            back_v[g][me] = o_v[g][me]
            send_back(lax.rem(ep + ROW_BLOCKS - 1, ROW_BLOCKS))

    chunk_count, group_count = iter(range(CHUNKS)), iter((0, 0, 1, 1))
    for step in STEPS:
        if step == "R":
            receive_next()
        elif step == "H":
            hidden_chunk(next(chunk_count))
        else:
            finish(next(group_count), int(step == "f"))

    every = pl.ds(0, ffn)
    for p in range(n_z - 1):
        for k in range(2):
            gate_up_copy(k, p, every, grecv.at[0, k, z]).wait_send()
        for g in range(2):
            for q in range(DOWN_SPLIT):
                down_copy(g, q, p).wait_send()
        if n_rep > 1:
            gate_up_pass(peers[p], rep, every, gpass_recv.at[0, peers[p]]).wait_send()
            for g in range(2):
                for q in range(DOWN_SPLIT):
                    down_pass(g, q, peers[p], rep).wait_send()

    scale = jnp.transpose(jnp.broadcast_to(gate_v[...], (LANE, tok_count)))
    low_lanes = lax.broadcasted_iota(jnp.int32, (tok_count, LANE), 1) < HALF
    mixed = []

    def piece(half):
        src, j = divmod(half, part // HALF)
        g, start = (0, src * LANE) if j < 2 else (1, (src // 2) * LANE)
        return mixed[g][:, start:start + LANE], j if j < 2 else src % 2

    def put(t):
        (low, low_at), (high, high_at) = piece(2 * t), piece(2 * t + 1)
        low = low if low_at == 0 else pltpu.roll(low, HALF, 1)
        high = high if high_at == 1 else pltpu.roll(high, HALF, 1)
        cols = slice(t * LANE, (t + 1) * LANE)
        value = jnp.where(low_lanes, low, high)
        out_ref[:, cols] = (tok_v[:, cols].astype(jnp.float32) + scale * value).astype(jnp.bfloat16)

    only_first = [t for t in range(dim // LANE) if (2 * t) % 3 < 2 and (2 * t + 1) % 3 < 2]
    for g in range(2):
        for_others(lambda s, g=g: back_copy(g, s, s).wait())
        mixed.append(jnp.dot(sel_v[...], back_v[g][...].reshape(slots, n_z * group_rows[g][1]),
                             preferred_element_type=jnp.float32))
        for t in range(dim // LANE):
            if (t in only_first) == (g == 0):
                put(t)


def solution(mesh):
    n_rep, n_ep, n_z = mesh.shape["rep"], mesh.shape["ep"], mesh.shape["fsdp"]
    row_spec = P(("rep", "ep", "fsdp"), None)

    def device_step(tokens, expert_idx, gates, w_gate, w_up, w_down):
        tok_count, top_k = expert_idx.shape
        n_local, part, ffn = w_gate.shape
        dim = tokens.shape[1]
        assert top_k == 1 and n_local == n_z and n_ep == ROW_BLOCKS and n_z == 4 and part == LANE + HALF and n_rep <= 2
        n_dev = n_ep * n_z
        cap = (2 * tok_count + n_dev - 1) // n_dev
        slots = n_dev * cap
        any_spec = pl.BlockSpec(memory_space=pl.ANY)
        dma, bf16 = pltpu.SemaphoreType.DMA, jnp.bfloat16
        return pl.pallas_call(
            functools.partial(moe_kernel, n_rep, n_ep, n_z, cap),
            out_shape=pltpu.VMEM((tok_count, dim), bf16),
            in_specs=[any_spec, any_spec, any_spec, any_spec, any_spec, any_spec],
            out_specs=pl.BlockSpec(memory_space=pltpu.VMEM),
            scratch_shapes=[
                pltpu.VMEM((1, tok_count), jnp.int32),
                pltpu.VMEM((1, tok_count), jnp.float32),
                pltpu.VMEM((tok_count, dim), bf16),
                pltpu.VMEM((n_dev, cap, dim), bf16),
                pltpu.VMEM((n_dev, cap, dim), bf16),
                pltpu.VMEM((2, n_z * part, ffn), bf16),
                pltpu.VMEM((n_z * LANE, ffn), bf16),
                pltpu.VMEM((n_z * HALF, ffn), bf16),
                pltpu.VMEM((slots, ffn), bf16),
                pltpu.VMEM((n_dev, cap, n_z * LANE), bf16),
                pltpu.VMEM((n_dev, cap, n_z * HALF), bf16),
                pltpu.VMEM((n_dev, cap, n_z * LANE), bf16),
                pltpu.VMEM((n_dev, cap, n_z * HALF), bf16),
                pltpu.VMEM((tok_count, slots), bf16),
                dma((3,)), dma((4,)),
                dma((2, n_z - 1)), dma((CHUNKS, 2, n_z)), dma((n_z,)), dma((CHUNKS, n_z)),
                dma((2, DOWN_SPLIT, n_z - 1)), dma((2, DOWN_SPLIT, n_z)), dma((2, DOWN_SPLIT, n_z)), dma((2, DOWN_SPLIT, n_z)),
                dma((n_dev,)), dma((n_dev,)), dma((2, n_dev)), dma((2, n_dev)),
            ],
            compiler_params=pltpu.CompilerParams(
                collective_id=0, has_side_effects=True, vmem_limit_bytes=60 * 1024 * 1024),
            cost_estimate=pl.CostEstimate(
                flops=6 * slots * dim * ffn, bytes_accessed=6 * dim * ffn, transcendentals=slots * ffn),
        )(expert_idx.reshape(1, tok_count), gates.reshape(1, tok_count), tokens, w_gate, w_up, jnp.swapaxes(w_down, 1, 2))

    return jax.shard_map(
        device_step, mesh=mesh,
        in_specs=(row_spec, row_spec, row_spec, P("ep", "fsdp", None), P("ep", "fsdp", None), P("ep", None, "fsdp")),
        out_specs=row_spec, check_vma=False)
```
